16 devices in a mesh: data: 4 (over z, y), stage: 4 (over x, core).
Axes of the slice: x: 2, y: 2, z: 2, core: 2. Of those that a mesh axis runs over, the one named last changes fastest.
Arguments:
- x_in: bfloat16 [128, 256, 768], P('data'), parts along dimension 0
- y_target: bfloat16 [128, 256, 768], P('data'), parts along dimension 0
- w_up: bfloat16 [4, 768, 3072], P('stage')
- w_down: bfloat16 [4, 3072, 768], P('stage')
- gain: float32 [4, 768], P('stage')
Outputs:
- output 1: float32 [4], P('data'), parts along dimension 0
- output 2: float32 [16, 768, 3072], P(('data', 'stage')), parts along dimension 0
- output 3: float32 [16, 3072, 768], P(('data', 'stage')), parts along dimension 0
- output 4: float32 [16, 768], P(('data', 'stage')), parts along dimension 0
There are 4 independent parts. The reference program is written for one: setup_inputs(seed, part) draws one part's arguments, and reference() takes and returns one part's arrays. A program takes and returns all parts, laid end to end along the dimension named above; an argument that names none is the same for every part.
All inputs are finite; a program needn't handle non-finite values.
Results may differ from the reference program's by a relative error of at most 0.0053043.
Values are sent between devices in bfloat16 or wider.
A program may use at most 1 GiB of HBM per device.

```python
import jax
import jax.numpy as jnp
from jax import lax

D_MODEL = 768
D_FF = 3072
NUM_MICRO = 32
MICRO_TOKENS = 256
NUM_LAYERS = 4
NORM_EPS = 1e-6


def setup_inputs(seed: int = 0, part: int = 0) -> dict:
    base_key = jax.random.key(seed)
    part_key = jax.random.fold_in(base_key, part)
    key_x, key_y = jax.random.split(part_key, 2)
    key_up, key_down, key_gain = jax.random.split(base_key, 3)
    act_shape = (NUM_MICRO, MICRO_TOKENS, D_MODEL)
    x_in = jax.random.normal(key_x, act_shape, jnp.float32).astype(jnp.bfloat16)
    y_target = jax.random.normal(key_y, act_shape, jnp.float32).astype(jnp.bfloat16)
    w_up = (jax.random.normal(key_up, (NUM_LAYERS, D_MODEL, D_FF), jnp.float32) * D_MODEL ** -0.5).astype(jnp.bfloat16)
    w_down = (jax.random.normal(key_down, (NUM_LAYERS, D_FF, D_MODEL), jnp.float32) * D_FF ** -0.5).astype(jnp.bfloat16)
    gain = 1.0 + 0.3 * jax.random.normal(key_gain, (NUM_LAYERS, D_MODEL), jnp.float32)
    return {"x_in": x_in, "y_target": y_target, "w_up": w_up, "w_down": w_down, "gain": gain}


def layer_forward(x_act, w_up, w_down, gain_vec):
    x_f = x_act.astype(jnp.float32)
    inv_rms = lax.rsqrt(jnp.mean(x_f * x_f, axis=-1, keepdims=True) + NORM_EPS)
    normed = (x_f * inv_rms * gain_vec).astype(jnp.bfloat16).astype(jnp.float32)
    pre_act = jnp.dot(normed, w_up, preferred_element_type=jnp.float32)
    hidden = jax.nn.gelu(pre_act).astype(jnp.bfloat16).astype(jnp.float32)
    update = jnp.dot(hidden, w_down, preferred_element_type=jnp.float32)
    return (x_f + update).astype(jnp.bfloat16)


def micro_loss(weights, x_micro, y_micro):
    def layer_step(x_act, layer_w):
        return jax.checkpoint(layer_forward)(x_act, layer_w[0], layer_w[1], layer_w[2]), None
    h_out, _ = lax.scan(layer_step, x_micro, weights)
    delta_out = h_out.astype(jnp.float32) - y_micro.astype(jnp.float32)
    return jnp.sum(delta_out * delta_out) / (NUM_MICRO * MICRO_TOKENS * D_MODEL)


def reference(x_in, y_target, w_up, w_down, gain):
    weights = (w_up.astype(jnp.float32), w_down.astype(jnp.float32), gain)
    grad_fn = jax.value_and_grad(micro_loss)

    def micro_step(acc_carry, micro_pair):
        loss_val, grad_set = grad_fn(weights, micro_pair[0], micro_pair[1])
        return (acc_carry[0] + loss_val, acc_carry[1] + grad_set[0], acc_carry[2] + grad_set[1], acc_carry[3] + grad_set[2]), None

    init_carry = (jnp.zeros((), jnp.float32), jnp.zeros_like(weights[0]), jnp.zeros_like(weights[1]), jnp.zeros_like(gain))
    totals, _ = lax.scan(micro_step, init_carry, (x_in, y_target))
    return totals[0].reshape(1), totals[1], totals[2], totals[3]
```

```python
import functools

import jax
import jax.numpy as jnp
from jax import lax
from jax.experimental import pallas as pl
from jax.experimental.pallas import tpu as pltpu
from jax.sharding import PartitionSpec as P

MESH = pl.DeviceIdType.MESH
F32 = jnp.float32
BF16 = jnp.bfloat16
NORM_EPS = 1e-6
STAGES = 4
LAG = 3
RING = 12
COLS = 512
ROWS = 64
NT = (((1,), (1,)), ((), ()))
GELU_C = 0.7978845608028654
GELU_A = 0.044715


def pipeline_kernel(x_hbm, y_hbm, w1_hbm, w2_hbm, gain_ref,
                    n_hbm, a_hbm, du_hbm, g_hbm, d_hbm, gg_ref, loss_ref,
                    w1, w2, xring, gring, xsend, gsend, nbuf, abuf, dbuf, dubuf, ybuf, gnbuf, lbuf,
                    wsem, xrecv, grecv, xsem, gsem, nsem, asem, dosem, dusem, ghsem, disem, ysem, lsend, lrecv):
    micro, tokens, width = x_hbm.shape
    hidden = w1.shape[1]
    stage = lax.axis_index("stage")
    first = stage == 0
    last = stage == STAGES - 1
    lag = LAG * (STAGES - 1 - stage)
    scale = 1.0 / (micro * tokens * width)

    def at_stage(pos):
        return {"stage": pos}

    def copy_w1():
        return pltpu.make_async_copy(w1_hbm.at[0], w1, wsem.at[0])

    def copy_w2():
        return pltpu.make_async_copy(w2_hbm.at[0], w2, wsem.at[1])

    def load_x(i):
        slot = lax.rem(i, RING)
        return pltpu.make_async_copy(x_hbm.at[i], xring.at[slot], xrecv.at[slot])

    def load_y(i):
        return pltpu.make_async_copy(y_hbm.at[i], ybuf.at[lax.rem(i, 2)], ysem.at[lax.rem(i, 2)])

    def send_x(i):
        return pltpu.make_async_remote_copy(
            src_ref=xsend.at[lax.rem(i, 2)], dst_ref=xring.at[lax.rem(i, RING)], send_sem=xsem.at[lax.rem(i, 2)],
            recv_sem=xrecv.at[lax.rem(i, RING)], device_id=at_stage(lax.rem(stage + 1, STAGES)), device_id_type=MESH)

    def send_g(i):
        return pltpu.make_async_remote_copy(
            src_ref=gsend.at[lax.rem(i, 2)], dst_ref=gring.at[lax.rem(i, RING)], send_sem=gsem.at[lax.rem(i, 2)],
            recv_sem=grecv.at[lax.rem(i, RING)], device_id=at_stage(lax.rem(stage + STAGES - 1, STAGES)),
            device_id_type=MESH)

    def save_n(i):
        return pltpu.make_async_copy(nbuf.at[lax.rem(i, 2)], n_hbm.at[i], nsem.at[lax.rem(i, 2)])

    def save_a(i):
        return pltpu.make_async_copy(abuf.at[lax.rem(i, 2)], a_hbm.at[i], asem.at[lax.rem(i, 2)])

    def save_d(i):
        return pltpu.make_async_copy(dbuf.at[lax.rem(i, 2)], d_hbm.at[i], dosem.at[lax.rem(i, 2)])

    def load_d(i):
        return pltpu.make_async_copy(d_hbm.at[i], dbuf.at[2 + lax.rem(i, 2)], disem.at[lax.rem(i, 2)])

    def save_du(i):
        return pltpu.make_async_copy(dubuf.at[lax.rem(i, 2)], du_hbm.at[i], dusem.at[lax.rem(i, 2)])

    def save_g(i):
        return pltpu.make_async_copy(gring.at[lax.rem(i, RING)], g_hbm.at[i], ghsem)

    copy_w1().start()
    copy_w2().start()

    @pl.when(first)
    def _():
        load_x(0).start()

    @pl.when(last)
    def _():
        load_y(0).start()

    barrier = pltpu.get_barrier_semaphore()
    for step in range(1, STAGES):
        pl.semaphore_signal(barrier, inc=1, device_id=at_stage(lax.rem(stage + step, STAGES)), device_id_type=MESH)
    pl.semaphore_wait(barrier, STAGES - 1)

    gg_ref[...] = jnp.zeros_like(gg_ref)
    lbuf[...] = jnp.zeros_like(lbuf)
    copy_w1().wait()
    copy_w2().wait()

    def forward(i):
        slot = lax.rem(i, RING)
        two = lax.rem(i, 2)

        @pl.when(first)
        def _():
            load_x(i).wait()

            @pl.when(i + 1 < micro)
            def _():
                load_x(i + 1).start()

        @pl.when(jnp.logical_not(first))
        def _():
            send_x(i).wait_recv()

        gain = gain_ref[...]
        for row in range(0, tokens, ROWS):
            x_f = xring[slot, row:row + ROWS, :].astype(F32)
            inv = lax.rsqrt(jnp.mean(x_f * x_f, axis=-1, keepdims=True) + NORM_EPS)
            nbuf[two, row:row + ROWS, :] = (x_f * inv * gain).astype(BF16)
        save_n(i).start()
        for col in range(0, hidden, COLS):
            u = jnp.dot(nbuf[two], w1[:, col:col + COLS], preferred_element_type=F32)
            u_sq = u * u
            th = jnp.tanh(u * (GELU_C + (GELU_C * GELU_A) * u_sq))
            h = 0.5 * th + 0.5
            abuf[two, :, col:col + COLS] = (u * h).astype(BF16)
            slope = u * (2.0 * GELU_C + (6.0 * GELU_C * GELU_A) * u_sq)
            dbuf[two, :, col:col + COLS] = h + (h - h * h) * slope
        save_a(i).start()

        @pl.when(jnp.logical_not(last))
        def _():
            save_d(i).start()

        update = jnp.dot(abuf[two], w2[...], preferred_element_type=F32)
        xsend[two] = (xring[slot].astype(F32) + update).astype(BF16)

        @pl.when(jnp.logical_not(last))
        def _():
            send_x(i).start()

        @pl.when(last)
        def _():
            load_y(i).wait()

            @pl.when(i + 1 < micro)
            def _():
                load_y(i + 1).start()

            for row in range(0, tokens, ROWS):
                delta = xsend[two, row:row + ROWS, :].astype(F32) - ybuf[two, row:row + ROWS, :].astype(F32)
                gring[slot, row:row + ROWS, :] = ((2.0 * scale) * delta).astype(BF16)
                lbuf[...] += jnp.sum((delta * delta).reshape(ROWS // 8, 8, width), axis=0)

    def backward(j):
        slot = lax.rem(j, RING)
        two = lax.rem(j, 2)
        d_slot = jnp.where(last, two, 2 + two)

        @pl.when(jnp.logical_not(last))
        def _():
            load_d(j).wait()
            send_g(j).wait_recv()

        save_g(j).start()
        for col in range(0, hidden, COLS):
            ga = lax.dot_general(gring[slot], w2[col:col + COLS, :], NT, preferred_element_type=F32)
            ga = ga.astype(BF16).astype(F32)
            dubuf[two, :, col:col + COLS] = (ga * dbuf[d_slot, :, col:col + COLS]).astype(BF16)
        save_du(j).start()
        gnbuf[...] = lax.dot_general(dubuf[two], w1[...], NT, preferred_element_type=F32).astype(BF16)
        gain = gain_ref[...]
        for row in range(0, tokens, ROWS):
            x_f = xring[slot, row:row + ROWS, :].astype(F32)
            inv = lax.rsqrt(jnp.mean(x_f * x_f, axis=-1, keepdims=True) + NORM_EPS)
            x_hat = x_f * inv
            gn = gnbuf[row:row + ROWS, :].astype(F32)
            gg_ref[...] += jnp.sum((gn * x_hat).reshape(ROWS // 8, 8, width), axis=0)
            ghat = gn * gain
            gx = inv * (ghat - x_hat * jnp.mean(ghat * x_hat, axis=-1, keepdims=True))
            gsend[two, row:row + ROWS, :] = (gring[slot, row:row + ROWS, :].astype(F32) + gx).astype(BF16)

        @pl.when(jnp.logical_not(first))
        def _():
            send_g(j).start()

    def tick(t, carry):
        i = t
        j = t - lag

        @pl.when((i >= 2) & (i < micro + 2))
        def _():
            save_n(i - 2).wait()
            save_a(i - 2).wait()

            @pl.when(jnp.logical_not(last))
            def _():
                save_d(i - 2).wait()
                send_x(i - 2).wait_send()

        @pl.when((j >= 1) & (j < micro + 1))
        def _():
            save_g(j - 1).wait()

        @pl.when((j >= 2) & (j < micro + 2))
        def _():
            save_du(j - 2).wait()

            @pl.when(jnp.logical_not(first))
            def _():
                send_g(j - 2).wait_send()

        @pl.when(i < micro)
        def _():
            forward(i)

        @pl.when(jnp.logical_not(last) & (j + 1 >= 0) & (j + 1 < micro))
        def _():
            load_d(j + 1).start()

        @pl.when((j >= 0) & (j < micro))
        def _():
            backward(j)

        return carry

    lax.fori_loop(0, micro + LAG * (STAGES - 1) + 2, tick, 0)

    def send_loss(pos):
        return pltpu.make_async_remote_copy(
            src_ref=lbuf, dst_ref=lbuf, send_sem=lsend.at[pos], recv_sem=lrecv, device_id=at_stage(pos),
            device_id_type=MESH)

    @pl.when(last)
    def _():
        for pos in range(STAGES - 1):
            send_loss(pos).start()
        for pos in range(STAGES - 1):
            send_loss(pos).wait_send()

    @pl.when(jnp.logical_not(last))
    def _():
        send_loss(0).wait_recv()

    loss_ref[...] = lbuf[...]


def run_pipeline(x_in, y_target, w_up, w_down, gain):
    micro, tokens, width = x_in.shape
    hidden = w_up.shape[2]
    any_spec = pl.BlockSpec(memory_space=pl.ANY)
    vmem_spec = pl.BlockSpec(memory_space=pltpu.VMEM)
    dma = pltpu.SemaphoreType.DMA
    return pl.pallas_call(
        pipeline_kernel,
        out_shape=(
            jax.ShapeDtypeStruct((micro, tokens, width), BF16),
            jax.ShapeDtypeStruct((micro, tokens, hidden), BF16),
            jax.ShapeDtypeStruct((micro, tokens, hidden), BF16),
            jax.ShapeDtypeStruct((micro, tokens, width), BF16),
            jax.ShapeDtypeStruct((micro, tokens, hidden), F32),
            jax.ShapeDtypeStruct((8, width), F32),
            jax.ShapeDtypeStruct((8, width), F32),
        ),
        in_specs=[any_spec, any_spec, any_spec, any_spec, vmem_spec],
        out_specs=(any_spec, any_spec, any_spec, any_spec, any_spec, vmem_spec, vmem_spec),
        scratch_shapes=[
            pltpu.VMEM((width, hidden), BF16),
            pltpu.VMEM((hidden, width), BF16),
            pltpu.VMEM((RING, tokens, width), BF16),
            pltpu.VMEM((RING, tokens, width), BF16),
            pltpu.VMEM((2, tokens, width), BF16),
            pltpu.VMEM((2, tokens, width), BF16),
            pltpu.VMEM((2, tokens, width), BF16),
            pltpu.VMEM((2, tokens, hidden), BF16),
            pltpu.VMEM((4, tokens, hidden), F32),
            pltpu.VMEM((2, tokens, hidden), BF16),
            pltpu.VMEM((2, tokens, width), BF16),
            pltpu.VMEM((tokens, width), BF16),
            pltpu.VMEM((8, width), F32),
            dma((2,)), dma((RING,)), dma((RING,)), dma((2,)), dma((2,)), dma((2,)), dma((2,)), dma((2,)), dma((2,)),
            dma, dma((2,)), dma((2,)), dma((STAGES - 1,)), dma,
        ],
        compiler_params=pltpu.CompilerParams(
            collective_id=0, has_side_effects=True, vmem_limit_bytes=67043328),
        cost_estimate=pl.CostEstimate(
            flops=8 * micro * tokens * width * hidden, transcendentals=micro * tokens * hidden,
            bytes_accessed=16 * micro * tokens * hidden),
        name="pipeline",
    )(x_in, y_target, w_up, w_down, gain)


def solution(mesh):
    def device_step(x_in, y_target, w_up, w_down, gain):
        micro, tokens, width = x_in.shape
        hidden = w_up.shape[2]
        n_all, a_all, du_all, g_all, _, gain_rows, loss_rows = run_pipeline(x_in, y_target, w_up, w_down, gain)
        rows = micro * tokens
        contract = (((0,), (0,)), ((), ()))
        grad_up = lax.dot_general(n_all.reshape(rows, width), du_all.reshape(rows, hidden), contract,
                                  preferred_element_type=F32)
        grad_down = lax.dot_general(a_all.reshape(rows, hidden), g_all.reshape(rows, width), contract,
                                    preferred_element_type=F32)
        loss = jnp.sum(loss_rows) * (1.0 / (rows * width))
        grad_gain = jnp.sum(gain_rows, axis=0, keepdims=True)
        return loss.reshape(1), grad_up[None], grad_down[None], grad_gain

    weight_spec = P("stage", None, None)
    grad_spec = P(("data", "stage"), None, None)
    return jax.shard_map(
        device_step, mesh=mesh,
        in_specs=(P("data", None, None), P("data", None, None), weight_spec, weight_spec, P("stage", None)),
        out_specs=(P("data"), grad_spec, grad_spec, P(("data", "stage"), None)), check_vma=False)
```

```python
import functools

import jax
import jax.numpy as jnp
from jax import lax
from jax.experimental import pallas as pl
from jax.experimental.pallas import tpu as pltpu
from jax.sharding import PartitionSpec as P

MESH = pl.DeviceIdType.MESH
F32 = jnp.float32
BF16 = jnp.bfloat16
NORM_EPS = 1e-6
STAGES = 4
LAG = 3
RING = 13
COLS = 256
OUTC = 256
HALF = 6
ORDER = (
    [step for k in range(HALF) for step in (("G", 2 * k), ("G", 2 * k + 1), ("E", k))]
    + [step for k in range(HALF) for step in (("N", 2 * k), ("E", HALF + k), ("N", 2 * k + 1))]
    + [("B", 0), ("U", 0), ("U", 1), ("U", 2)]
)
ROWS = 64
NT = (((1,), (1,)), ((), ()))
GELU_C = 0.7978845608028654
GELU_A = 0.044715


def pipeline_kernel(x_hbm, y_hbm, w1_hbm, w2_hbm, gain_ref,
                    n_hbm, a_hbm, du_hbm, g_hbm, d_hbm, gg_ref, loss_ref,
                    w1, w2, xring, gring, xsend, gsend, nbuf, abuf, dbuf, dubuf, ybuf, gnbuf, lbuf,
                    wsem, xrecv, grecv, xsem, gsem, nsem, asem, dosem, dusem, ghsem, disem, ysem, lsend, lrecv):
    micro, tokens, width = x_hbm.shape
    hidden = w1.shape[1]
    stage = lax.axis_index("stage")
    first = stage == 0
    last = stage == STAGES - 1
    lag = LAG * (STAGES - 1 - stage) + 1 + jnp.where(stage < STAGES // 2, 1, 0)
    scale = 1.0 / (micro * tokens * width)

    def at_stage(pos):
        return {"stage": pos}

    def copy_w1():
        return pltpu.make_async_copy(w1_hbm.at[0], w1, wsem.at[0])

    def copy_w2():
        return pltpu.make_async_copy(w2_hbm.at[0], w2, wsem.at[1])

    def load_x(i):
        slot = lax.rem(i, RING)
        return pltpu.make_async_copy(x_hbm.at[i], xring.at[slot], xrecv.at[slot])

    def load_y(i):
        return pltpu.make_async_copy(y_hbm.at[i], ybuf.at[lax.rem(i, 2)], ysem.at[lax.rem(i, 2)])

    def send_x(i):
        return pltpu.make_async_remote_copy(
            src_ref=xsend.at[lax.rem(i, 2)], dst_ref=xring.at[lax.rem(i, RING)], send_sem=xsem.at[lax.rem(i, 2)],
            recv_sem=xrecv.at[lax.rem(i, RING)], device_id=at_stage(lax.rem(stage + 1, STAGES)), device_id_type=MESH)

    def send_g(i):
        return pltpu.make_async_remote_copy(
            src_ref=gsend.at[lax.rem(i, 2)], dst_ref=gring.at[lax.rem(i, RING)], send_sem=gsem.at[lax.rem(i, 2)],
            recv_sem=grecv.at[lax.rem(i, RING)], device_id=at_stage(lax.rem(stage + STAGES - 1, STAGES)),
            device_id_type=MESH)

    def save_n(i):
        return pltpu.make_async_copy(nbuf.at[lax.rem(i, 2)], n_hbm.at[i], nsem.at[lax.rem(i, 2)])

    def save_a(i):
        return pltpu.make_async_copy(abuf.at[lax.rem(i, 2)], a_hbm.at[i], asem.at[lax.rem(i, 2)])

    def save_d(i):
        return pltpu.make_async_copy(dbuf.at[lax.rem(i, 2)], d_hbm.at[i], dosem.at[lax.rem(i, 2)])

    def load_d(i):
        return pltpu.make_async_copy(d_hbm.at[i], dbuf.at[2 + lax.rem(i, 2)], disem.at[lax.rem(i, 2)])

    def save_du(i):
        return pltpu.make_async_copy(dubuf.at[lax.rem(i, 2)], du_hbm.at[i], dusem.at[lax.rem(i, 2)])

    def save_g(i):
        slot = jnp.where(last, RING + lax.rem(i, 2), lax.rem(i, RING))
        return pltpu.make_async_copy(gring.at[slot], g_hbm.at[i], ghsem)

    copy_w1().start()
    copy_w2().start()

    @pl.when(first)
    def _():
        load_x(0).start()

    load_y(0).start()
    barrier = pltpu.get_barrier_semaphore()
    for step in range(1, STAGES):
        pl.semaphore_signal(barrier, inc=1, device_id=at_stage(lax.rem(stage + step, STAGES)), device_id_type=MESH)
    pl.semaphore_wait(barrier, STAGES - 1)

    gg_ref[...] = jnp.zeros_like(gg_ref)
    lbuf[...] = jnp.zeros_like(lbuf)
    copy_w1().wait()
    copy_w2().wait()

    def normalize(i, slot, two):
        gain = gain_ref[...]
        for row in range(0, tokens, ROWS):
            x_f = xring[slot, row:row + ROWS, :].astype(F32)
            inv = lax.rsqrt(jnp.mean(x_f * x_f, axis=-1, keepdims=True) + NORM_EPS)
            nbuf[two, row:row + ROWS, :] = (x_f * inv * gain).astype(BF16)

    def expand(two, col):
        u = jnp.dot(nbuf[two], w1[:, col:col + COLS], preferred_element_type=F32)
        u_sq = u * u
        th = jnp.tanh(u * (GELU_C + (GELU_C * GELU_A) * u_sq))
        h = 0.5 * th + 0.5
        abuf[two, :, col:col + COLS] = (u * h).astype(BF16)
        slope = u * (2.0 * GELU_C + (6.0 * GELU_C * GELU_A) * u_sq)
        dbuf[two, :, col:col + COLS] = h + (h - h * h) * slope

    def finish_forward(slot, two, ocol, update):
        out = (xring[slot, :, ocol].astype(F32) + update).astype(BF16)
        xsend[two, :, ocol] = out
        delta = out.astype(F32) - ybuf[two, :, ocol].astype(F32)
        gring[RING + two, :, ocol] = ((2.0 * scale) * delta).astype(BF16)
        lbuf[:, ocol] += jnp.sum((delta * delta).reshape(tokens // 8, 8, OUTC), axis=0)

    def grad_hidden(g_slot, d_slot, two, col):
        ga = lax.dot_general(gring[g_slot], w2[col:col + COLS, :], NT, preferred_element_type=F32)
        ga = ga.astype(BF16).astype(F32)
        dubuf[two, :, col:col + COLS] = (ga * dbuf[d_slot, :, col:col + COLS]).astype(BF16)

    def finish_backward(slot, g_slot, two, gn_all):
        gnbuf[...] = gn_all.astype(BF16)
        gain = gain_ref[...]
        for row in range(0, tokens, ROWS):
            x_f = xring[slot, row:row + ROWS, :].astype(F32)
            inv = lax.rsqrt(jnp.mean(x_f * x_f, axis=-1, keepdims=True) + NORM_EPS)
            x_hat = x_f * inv
            gn = gnbuf[row:row + ROWS, :].astype(F32)
            gg_ref[...] += jnp.sum((gn * x_hat).reshape(ROWS // 8, 8, width), axis=0)
            ghat = gn * gain
            gx = inv * (ghat - x_hat * jnp.mean(ghat * x_hat, axis=-1, keepdims=True))
            gsend[two, row:row + ROWS, :] = (gring[g_slot, row:row + ROWS, :].astype(F32) + gx).astype(BF16)

    def compute(do_f, do_b, i, j):
        f_slot, f_two = lax.rem(i, RING), lax.rem(i, 2)
        b_slot, b_two = lax.rem(j, RING), lax.rem(j, 2)
        d_slot = jnp.where(last, b_two, 2 + b_two)
        g_slot = jnp.where(last, RING + b_two, b_slot)
        blocks = range(hidden // COLS)
        if do_f:
            normalize(i, f_slot, f_two)
        gn_all = None
        for kind, k in ORDER:
            if kind == "E" and do_f:
                expand(f_two, k * COLS)
            if kind == "G" and do_b:
                grad_hidden(g_slot, d_slot, b_two, k * COLS)
            if kind == "N" and do_b:
                part = lax.dot_general(dubuf[b_two, :, k * COLS:(k + 1) * COLS], w1[:, k * COLS:(k + 1) * COLS], NT,
                                       preferred_element_type=F32)
                gn_all = part if gn_all is None else gn_all + part
            if kind == "B" and do_b:
                finish_backward(b_slot, g_slot, b_two, gn_all)
            if kind == "U" and do_f:
                ocol = slice(k * OUTC, (k + 1) * OUTC)
                update = jnp.dot(abuf[f_two], w2[:, ocol], preferred_element_type=F32)
                finish_forward(f_slot, f_two, ocol, update)

    def before_forward(i):
        @pl.when(first)
        def _():
            load_x(i).wait()

            @pl.when(i + 1 < micro)
            def _():
                load_x(i + 1).start()

        @pl.when(jnp.logical_not(first))
        def _():
            send_x(i).wait_recv()

        load_y(i).wait()

        @pl.when(i + 1 < micro)
        def _():
            load_y(i + 1).start()

    def after_forward(i):
        save_n(i).start()
        save_a(i).start()

        @pl.when(jnp.logical_not(last))
        def _():
            save_d(i).start()
            send_x(i).start()

    def before_backward(j):
        @pl.when(jnp.logical_not(last))
        def _():
            load_d(j).wait()
            send_g(j).wait_recv()

        save_g(j).start()

    def after_backward(j):
        save_du(j).start()

        @pl.when(jnp.logical_not(first))
        def _():
            send_g(j).start()

    def tick(t, carry):
        i = t
        j = t - lag
        f_on = i < micro
        b_on = (j >= 0) & (j < micro)

        @pl.when((i >= 2) & (i < micro + 2))
        def _():
            save_n(i - 2).wait()
            save_a(i - 2).wait()

            @pl.when(jnp.logical_not(last))
            def _():
                save_d(i - 2).wait()
                send_x(i - 2).wait_send()

        @pl.when((j >= 1) & (j < micro + 1))
        def _():
            save_g(j - 1).wait()

        @pl.when((j >= 2) & (j < micro + 2))
        def _():
            save_du(j - 2).wait()

            @pl.when(jnp.logical_not(first))
            def _():
                send_g(j - 2).wait_send()

        @pl.when(f_on)
        def _():
            before_forward(i)

        @pl.when(b_on)
        def _():
            before_backward(j)

        @pl.when(jnp.logical_not(last) & (j + 1 >= 0) & (j + 1 < micro))
        def _():
            load_d(j + 1).start()

        @pl.when(f_on & b_on)
        def _():
            compute(True, True, i, j)

        @pl.when(f_on & jnp.logical_not(b_on))
        def _():
            compute(True, False, i, j)

        @pl.when(b_on & jnp.logical_not(f_on))
        def _():
            compute(False, True, i, j)

        @pl.when(b_on)
        def _():
            after_backward(j)

        @pl.when(f_on)
        def _():
            after_forward(i)

        return carry

    lax.fori_loop(0, micro + LAG * (STAGES - 1) + 4, tick, 0)

    def send_loss(pos):
        return pltpu.make_async_remote_copy(
            src_ref=lbuf, dst_ref=lbuf, send_sem=lsend.at[pos], recv_sem=lrecv, device_id=at_stage(pos),
            device_id_type=MESH)

    @pl.when(last)
    def _():
        for pos in range(STAGES - 1):
            send_loss(pos).start()
        for pos in range(STAGES - 1):
            send_loss(pos).wait_send()

    @pl.when(jnp.logical_not(last))
    def _():
        send_loss(0).wait_recv()

    loss_ref[...] = lbuf[...]


def run_pipeline(x_in, y_target, w_up, w_down, gain):
    micro, tokens, width = x_in.shape
    hidden = w_up.shape[2]
    any_spec = pl.BlockSpec(memory_space=pl.ANY)
    vmem_spec = pl.BlockSpec(memory_space=pltpu.VMEM)
    dma = pltpu.SemaphoreType.DMA
    return pl.pallas_call(
        pipeline_kernel,
        out_shape=(
            jax.ShapeDtypeStruct((micro, tokens, width), BF16),
            jax.ShapeDtypeStruct((micro, tokens, hidden), BF16),
            jax.ShapeDtypeStruct((micro, tokens, hidden), BF16),
            jax.ShapeDtypeStruct((micro, tokens, width), BF16),
            jax.ShapeDtypeStruct((micro, tokens, hidden), F32),
            jax.ShapeDtypeStruct((8, width), F32),
            jax.ShapeDtypeStruct((8, width), F32),
        ),
        in_specs=[any_spec, any_spec, any_spec, any_spec, vmem_spec],
        out_specs=(any_spec, any_spec, any_spec, any_spec, any_spec, vmem_spec, vmem_spec),
        scratch_shapes=[
            pltpu.VMEM((width, hidden), BF16),
            pltpu.VMEM((hidden, width), BF16),
            pltpu.VMEM((RING, tokens, width), BF16),
            pltpu.VMEM((RING + 2, tokens, width), BF16),
            pltpu.VMEM((2, tokens, width), BF16),
            pltpu.VMEM((2, tokens, width), BF16),
            pltpu.VMEM((2, tokens, width), BF16),
            pltpu.VMEM((2, tokens, hidden), BF16),
            pltpu.VMEM((4, tokens, hidden), F32),
            pltpu.VMEM((2, tokens, hidden), BF16),
            pltpu.VMEM((2, tokens, width), BF16),
            pltpu.VMEM((tokens, width), BF16),
            pltpu.VMEM((8, width), F32),
            dma((2,)), dma((RING,)), dma((RING,)), dma((2,)), dma((2,)), dma((2,)), dma((2,)), dma((2,)), dma((2,)),
            dma, dma((2,)), dma((2,)), dma((STAGES - 1,)), dma,
        ],
        compiler_params=pltpu.CompilerParams(
            collective_id=0, has_side_effects=True,
            vmem_limit_bytes=67043328),
        cost_estimate=pl.CostEstimate(
            flops=8 * micro * tokens * width * hidden, transcendentals=micro * tokens * hidden,
            bytes_accessed=16 * micro * tokens * hidden),
        name="pipeline",
    )(x_in, y_target, w_up, w_down, gain)


def solution(mesh):
    def device_step(x_in, y_target, w_up, w_down, gain):
        micro, tokens, width = x_in.shape
        hidden = w_up.shape[2]
        n_all, a_all, du_all, g_all, _, gain_rows, loss_rows = run_pipeline(x_in, y_target, w_up, w_down, gain)
        rows = micro * tokens
        contract = (((0,), (0,)), ((), ()))
        grad_up = lax.dot_general(n_all.reshape(rows, width), du_all.reshape(rows, hidden), contract,
                                  preferred_element_type=F32)
        grad_down = lax.dot_general(a_all.reshape(rows, hidden), g_all.reshape(rows, width), contract,
                                    preferred_element_type=F32)
        loss = jnp.sum(loss_rows) * (1.0 / (rows * width))
        grad_gain = jnp.sum(gain_rows, axis=0, keepdims=True)
        return loss.reshape(1), grad_up[None], grad_down[None], grad_gain

    weight_spec = P("stage", None, None)
    grad_spec = P(("data", "stage"), None, None)
    return jax.shard_map(
        device_step, mesh=mesh,
        in_specs=(P("data", None, None), P("data", None, None), weight_spec, weight_spec, P("stage", None)),
        out_specs=(P("data"), grad_spec, grad_spec, P(("data", "stage"), None)), check_vma=False)
```

```python
import functools

import jax
import jax.numpy as jnp
from jax import lax
from jax.experimental import pallas as pl
from jax.experimental.pallas import tpu as pltpu
from jax.sharding import PartitionSpec as P

MESH = pl.DeviceIdType.MESH
F32 = jnp.float32
BF16 = jnp.bfloat16
NORM_EPS = 1e-6
STAGES = 4
LAG = 3
RING = 13
G_RING = 6
COLS = 256
WCOLS = 512
WIDE = 512
OUTC = 256
ORDER = [('G', 0), ('G', 1), ('E', 0), ('G', 2), ('G', 3), ('E', 1), ('G', 4), ('G', 5), ('E', 2), ('G', 6), ('G', 7), ('E', 3), ('G', 8), ('G', 9), ('E', 4), ('G', 10), ('G', 11), ('E', 5), ('N', 0), ('E', 6), ('N', 1), ('N', 2), ('E', 7), ('N', 3), ('N', 4), ('E', 8), ('N', 5), ('N', 6), ('E', 9), ('N', 7), ('N', 8), ('E', 10), ('N', 9), ('N', 10), ('E', 11), ('N', 11), ('B', 0), ('U', 0), ('U', 1), ('U', 2)]
ROWS = 64
NT = (((1,), (1,)), ((), ()))
GELU_C = 0.7978845608028654
GELU_A = 0.044715


def lag_of(stage):
    return LAG * (STAGES - 1 - stage) + 1 + jnp.where(stage < STAGES // 2, 1, 0)


def pipeline_kernel(x_hbm, y_hbm, w1_hbm, w2_hbm, gain_ref,
                    nt_hbm, a_hbm, du_hbm, gt_hbm, d_hbm, acc_hbm, gg_ref, loss_ref,
                    w1, w2, xring, gring, gsend, nbuf, ntbuf, gtbuf, abuf, dbuf, dubuf, ybuf, acc, wnt, wa, lbuf,
                    wsem, xrecv, grecv, xsem, gsem, ntsem, asem, dosem, dusem, gtsem, disem, ysem, wlsem, accsem,
                    lsend, lrecv, gfree):
    micro, tokens, width = x_hbm.shape
    hidden = w1.shape[1]
    stage = lax.axis_index("stage")
    first = stage == 0
    last = stage == STAGES - 1
    lag = lag_of(stage)
    scale = 1.0 / (micro * tokens * width)

    def at_stage(pos):
        return {"stage": pos}

    def copy_w1():
        return pltpu.make_async_copy(w1_hbm.at[0], w1, wsem.at[0])

    def copy_w2():
        return pltpu.make_async_copy(w2_hbm.at[0], w2, wsem.at[1])

    def load_x(i):
        slot = lax.rem(i, RING)
        return pltpu.make_async_copy(x_hbm.at[i], xring.at[slot], xrecv.at[slot])

    def load_y(i):
        return pltpu.make_async_copy(y_hbm.at[i], ybuf.at[lax.rem(i, 2)], ysem.at[lax.rem(i, 2)])

    def send_x(i):
        return pltpu.make_async_remote_copy(
            src_ref=gring.at[G_RING + lax.rem(i, 2)], dst_ref=xring.at[lax.rem(i, RING)], send_sem=xsem.at[lax.rem(i, 2)],
            recv_sem=xrecv.at[lax.rem(i, RING)], device_id=at_stage(lax.rem(stage + 1, STAGES)), device_id_type=MESH)

    def send_g(i):
        return pltpu.make_async_remote_copy(
            src_ref=gsend.at[lax.rem(i, 2)], dst_ref=gring.at[lax.rem(i, G_RING)], send_sem=gsem.at[lax.rem(i, 2)],
            recv_sem=grecv.at[lax.rem(i, G_RING)], device_id=at_stage(lax.rem(stage + STAGES - 1, STAGES)),
            device_id_type=MESH)

    def save_nt(i):
        return pltpu.make_async_copy(ntbuf.at[lax.rem(i, 2)], nt_hbm.at[i], ntsem.at[lax.rem(i, 2)])

    def save_a(i):
        return pltpu.make_async_copy(abuf.at[lax.rem(i, 2)], a_hbm.at[i], asem.at[lax.rem(i, 2)])

    def save_d(i):
        return pltpu.make_async_copy(dbuf.at[lax.rem(i, 2)], d_hbm.at[i], dosem.at[lax.rem(i, 2)])

    def load_d(i):
        return pltpu.make_async_copy(d_hbm.at[i], dbuf.at[2 + lax.rem(i, 2)], disem.at[lax.rem(i, 2)])

    def save_du(i):
        return pltpu.make_async_copy(dubuf.at[lax.rem(i, 2)], du_hbm.at[i], dusem.at[lax.rem(i, 2)])

    def save_gt(i):
        return pltpu.make_async_copy(gtbuf.at[lax.rem(i, 2)], gt_hbm.at[i], gtsem.at[lax.rem(i, 2)])

    def load_wnt(i):
        return pltpu.make_async_copy(nt_hbm.at[i], wnt, wlsem.at[0])

    def load_wa(i):
        return pltpu.make_async_copy(a_hbm.at[i], wa, wlsem.at[1])

    def save_acc():
        return pltpu.make_async_copy(acc, acc_hbm, accsem)

    copy_w1().start()
    copy_w2().start()

    @pl.when(first)
    def _():
        load_x(0).start()

    load_y(0).start()
    barrier = pltpu.get_barrier_semaphore()
    for step in range(1, STAGES):
        pl.semaphore_signal(barrier, inc=1, device_id=at_stage(lax.rem(stage + step, STAGES)), device_id_type=MESH)
    pl.semaphore_wait(barrier, STAGES - 1)

    gg_ref[...] = jnp.zeros_like(gg_ref)
    lbuf[...] = jnp.zeros_like(lbuf)

    def clear(row, carry):
        for part in range(2):
            acc[part, pl.ds(pl.multiple_of(row * 8, 8), 8), :] = jnp.zeros((8, hidden), F32)
        return carry

    lax.fori_loop(0, width // 8, clear, 0)
    copy_w1().wait()
    copy_w2().wait()

    def normalize(i, slot, two):
        gain = gain_ref[...]
        for row in range(0, tokens, ROWS):
            x_f = xring[slot, row:row + ROWS, :].astype(F32)
            inv = lax.rsqrt(jnp.mean(x_f * x_f, axis=-1, keepdims=True) + NORM_EPS)
            nbuf[row:row + ROWS, :] = (x_f * inv * gain).astype(BF16)
        ntbuf[two] = nbuf[...].T

    def expand(two, col):
        u = jnp.dot(nbuf[...], w1[:, col:col + COLS], preferred_element_type=F32)
        u_sq = u * u
        th = jnp.tanh(u * (GELU_C + (GELU_C * GELU_A) * u_sq))
        h = 0.5 * th + 0.5
        abuf[two, :, col:col + COLS] = (u * h).astype(BF16)
        slope = u * (2.0 * GELU_C + (6.0 * GELU_C * GELU_A) * u_sq)
        dbuf[two, :, col:col + COLS] = h + (h - h * h) * slope

    def finish_forward(slot, two, ocol, update):
        out = (xring[slot, :, ocol].astype(F32) + update).astype(BF16)
        delta = out.astype(F32) - ybuf[two, :, ocol].astype(F32)
        gring[G_RING + two, :, ocol] = jnp.where(last, ((2.0 * scale) * delta).astype(BF16), out)
        lbuf[:, ocol] += jnp.sum((delta * delta).reshape(tokens // 8, 8, OUTC), axis=0)

    def grad_hidden(g_slot, d_slot, two, col):
        ga = lax.dot_general(gring[g_slot], w2[col:col + COLS, :], NT, preferred_element_type=F32)
        ga = ga.astype(BF16).astype(F32)
        dubuf[two, :, col:col + COLS] = (ga * dbuf[d_slot, :, col:col + COLS]).astype(BF16)

    def finish_backward(slot, g_slot, two, gn_all):
        gsend[two] = gn_all.astype(BF16)
        gain = gain_ref[...]
        for row in range(0, tokens, ROWS):
            x_f = xring[slot, row:row + ROWS, :].astype(F32)
            inv = lax.rsqrt(jnp.mean(x_f * x_f, axis=-1, keepdims=True) + NORM_EPS)
            x_hat = x_f * inv
            gn = gsend[two, row:row + ROWS, :].astype(F32)
            gg_ref[...] += jnp.sum((gn * x_hat).reshape(ROWS // 8, 8, width), axis=0)
            ghat = gn * gain
            gx = inv * (ghat - x_hat * jnp.mean(ghat * x_hat, axis=-1, keepdims=True))
            gsend[two, row:row + ROWS, :] = (gring[g_slot, row:row + ROWS, :].astype(F32) + gx).astype(BF16)

    def compute(do_f, do_b, i, j):
        f_slot, f_two = lax.rem(i, RING), lax.rem(i, 2)
        b_slot, b_two = lax.rem(j, RING), lax.rem(j, 2)
        d_slot = jnp.where(last, b_two, 2 + b_two)
        g_slot = jnp.where(last, G_RING + b_two, lax.rem(j, G_RING))
        blocks = range(hidden // COLS)
        if do_f:
            normalize(i, f_slot, f_two)
        gn_all = None
        for kind, k in ORDER:
            if kind == "E" and do_f:
                expand(f_two, k * COLS)
            if kind == "G" and do_b:
                grad_hidden(g_slot, d_slot, b_two, k * COLS)
            if kind == "N" and do_b:
                part = lax.dot_general(dubuf[b_two, :, k * COLS:(k + 1) * COLS], w1[:, k * COLS:(k + 1) * COLS], NT,
                                       preferred_element_type=F32)
                gn_all = part if gn_all is None else gn_all + part
            if kind == "B" and do_b:
                gtbuf[b_two] = gring[g_slot].T
                finish_backward(b_slot, g_slot, b_two, gn_all)
            if kind == "U" and do_f:
                ocol = slice(k * OUTC, (k + 1) * OUTC)
                update = jnp.dot(abuf[f_two], w2[:, ocol], preferred_element_type=F32)
                finish_forward(f_slot, f_two, ocol, update)

    def weight_grads(j):
        two = lax.rem(j, 2)
        load_wnt(j).wait()
        load_wa(j).wait()
        for col in range(0, hidden, WCOLS):
            block = slice(col, col + WCOLS)
            acc[0, :, block] += jnp.dot(wnt[...], dubuf[two, :, block], preferred_element_type=F32)
            acc[1, :, block] += jnp.dot(gtbuf[two], wa[:, block], preferred_element_type=F32)

    def before_forward(i):
        @pl.when(first)
        def _():
            load_x(i).wait()

            @pl.when(i + 1 < micro)
            def _():
                load_x(i + 1).start()

        @pl.when(jnp.logical_not(first))
        def _():
            send_x(i).wait_recv()

        load_y(i).wait()

        @pl.when(i + 1 < micro)
        def _():
            load_y(i + 1).start()

    def after_forward(i):
        save_nt(i).start()
        save_a(i).start()

        @pl.when(jnp.logical_not(last))
        def _():
            save_d(i).start()
            send_x(i).start()

    def before_backward(j):
        @pl.when(jnp.logical_not(last))
        def _():
            load_d(j).wait()
            send_g(j).wait_recv()

    def after_backward(j):
        save_du(j).start()
        save_gt(j).start()

        @pl.when(jnp.logical_not(last) & (j < micro - G_RING))
        def _():
            pl.semaphore_signal(gfree, inc=1, device_id=at_stage(lax.rem(stage + 1, STAGES)), device_id_type=MESH)

        @pl.when(jnp.logical_not(first) & (j >= G_RING))
        def _():
            pl.semaphore_wait(gfree, 1)

        @pl.when(jnp.logical_not(first))
        def _():
            send_g(j).start()

    def tick(t, carry):
        i = t
        j = t - lag
        f_on = i < micro
        b_on = (j >= 0) & (j < micro)

        @pl.when((i >= 2) & (i < micro + 2))
        def _():
            save_nt(i - 2).wait()
            save_a(i - 2).wait()

            @pl.when(jnp.logical_not(last))
            def _():
                save_d(i - 2).wait()
                send_x(i - 2).wait_send()

        @pl.when((j >= 2) & (j < micro + 2))
        def _():
            save_du(j - 2).wait()
            save_gt(j - 2).wait()

            @pl.when(jnp.logical_not(first))
            def _():
                send_g(j - 2).wait_send()

        @pl.when(f_on)
        def _():
            before_forward(i)

        @pl.when(b_on)
        def _():
            before_backward(j)

        @pl.when(jnp.logical_not(last) & (j + 1 >= 0) & (j + 1 < micro))
        def _():
            load_d(j + 1).start()

        w_on = jnp.logical_not(f_on) & (j < micro - 1)

        @pl.when(w_on)
        def _():
            load_wnt(j).start()
            load_wa(j).start()

        @pl.when(j == micro - 1)
        def _():
            save_acc().start()

        @pl.when(f_on & b_on)
        def _():
            compute(True, True, i, j)

        @pl.when(f_on & jnp.logical_not(b_on))
        def _():
            compute(True, False, i, j)

        @pl.when(b_on & jnp.logical_not(f_on))
        def _():
            compute(False, True, i, j)

        @pl.when(b_on)
        def _():
            after_backward(j)

        @pl.when(f_on)
        def _():
            after_forward(i)

        @pl.when(w_on)
        def _():
            weight_grads(j)

        return carry

    lax.fori_loop(0, micro + LAG * (STAGES - 1) + 4, tick, 0)

    save_acc().wait()

    def send_loss(pos):
        return pltpu.make_async_remote_copy(
            src_ref=lbuf, dst_ref=lbuf, send_sem=lsend.at[pos], recv_sem=lrecv, device_id=at_stage(pos),
            device_id_type=MESH)

    @pl.when(last)
    def _():
        for pos in range(STAGES - 1):
            send_loss(pos).start()
        for pos in range(STAGES - 1):
            send_loss(pos).wait_send()

    @pl.when(jnp.logical_not(last))
    def _():
        send_loss(0).wait_recv()

    loss_ref[...] = lbuf[...]


def run_pipeline(x_in, y_target, w_up, w_down, gain):
    micro, tokens, width = x_in.shape
    hidden = w_up.shape[2]
    any_spec = pl.BlockSpec(memory_space=pl.ANY)
    vmem_spec = pl.BlockSpec(memory_space=pltpu.VMEM)
    dma = pltpu.SemaphoreType.DMA
    return pl.pallas_call(
        pipeline_kernel,
        out_shape=(
            jax.ShapeDtypeStruct((micro, width, tokens), BF16),
            jax.ShapeDtypeStruct((micro, tokens, hidden), BF16),
            jax.ShapeDtypeStruct((micro, tokens, hidden), BF16),
            jax.ShapeDtypeStruct((micro, width, tokens), BF16),
            jax.ShapeDtypeStruct((micro, tokens, hidden), F32),
            jax.ShapeDtypeStruct((2, width, hidden), F32),
            jax.ShapeDtypeStruct((8, width), F32),
            jax.ShapeDtypeStruct((8, width), F32),
        ),
        in_specs=[any_spec, any_spec, any_spec, any_spec, vmem_spec],
        out_specs=(any_spec, any_spec, any_spec, any_spec, any_spec, any_spec, vmem_spec, vmem_spec),
        scratch_shapes=[
            pltpu.VMEM((width, hidden), BF16),
            pltpu.VMEM((hidden, width), BF16),
            pltpu.VMEM((RING, tokens, width), BF16),
            pltpu.VMEM((G_RING + 2, tokens, width), BF16),
            pltpu.VMEM((2, tokens, width), BF16),
            pltpu.VMEM((tokens, width), BF16),
            pltpu.VMEM((2, width, tokens), BF16),
            pltpu.VMEM((2, width, tokens), BF16),
            pltpu.VMEM((2, tokens, hidden), BF16),
            pltpu.VMEM((4, tokens, hidden), F32),
            pltpu.VMEM((2, tokens, hidden), BF16),
            pltpu.VMEM((2, tokens, width), BF16),
            pltpu.VMEM((2, width, hidden), F32),
            pltpu.VMEM((width, tokens), BF16),
            pltpu.VMEM((tokens, hidden), BF16),
            pltpu.VMEM((8, width), F32),
            dma((2,)), dma((RING,)), dma((G_RING,)), dma((2,)), dma((2,)), dma((2,)), dma((2,)), dma((2,)), dma((2,)),
            dma((2,)), dma((2,)), dma((2,)), dma((2,)), dma, dma((STAGES - 1,)), dma, pltpu.SemaphoreType.REGULAR,
        ],
        compiler_params=pltpu.CompilerParams(
            collective_id=0, has_side_effects=True,
            vmem_limit_bytes=67043328),
        cost_estimate=pl.CostEstimate(
            flops=8 * micro * tokens * width * hidden, transcendentals=micro * tokens * hidden,
            bytes_accessed=16 * micro * tokens * hidden),
        name="pipeline",
    )(x_in, y_target, w_up, w_down, gain)


def weight_kernel(nt_hbm, gt_hbm, du_hbm, a_hbm, acc_hbm, up_hbm, down_hbm,
                  lhs, rhs, prev, up_out, down_out, lsem, rsem, psem, osem):
    micro, width, tokens = nt_hbm.shape
    hidden = du_hbm.shape[2]
    rounds = hidden // WIDE
    half = WIDE // 2
    cut = micro - lag_of(lax.axis_index("stage"))
    count = cut + 1

    def source(k):
        return jnp.where(k < cut, k, micro - 1)

    def load_lhs(part, k):
        return pltpu.make_async_copy((nt_hbm, gt_hbm)[part].at[source(k)], lhs.at[part, k], lsem.at[part, k])

    def load_rhs(part, pair, k):
        cols = pl.ds(pl.multiple_of(pair * WIDE, WIDE), WIDE)
        buf = lax.rem(pair, 2)
        return pltpu.make_async_copy((du_hbm, a_hbm)[part].at[source(k), :, cols], rhs.at[buf, k], rsem.at[buf, k])

    def load_prev(part, pair):
        cols = pl.ds(pl.multiple_of(pair * WIDE, WIDE), WIDE)
        buf = lax.rem(pair, 2)
        return pltpu.make_async_copy(acc_hbm.at[part, :, cols], prev.at[buf], psem.at[buf])

    def save(part, pair):
        start = pl.multiple_of(pair * WIDE, WIDE)
        buf = lax.rem(pair, 2)
        if part == 0:
            return pltpu.make_async_copy(up_out.at[buf], up_hbm.at[:, pl.ds(start, WIDE)], osem.at[0, buf])
        return pltpu.make_async_copy(down_out.at[buf], down_hbm.at[pl.ds(start, WIDE), :], osem.at[1, buf])

    def fetch(part, pair):
        load_prev(part, pair).start()

        def one(k, carry):
            load_rhs(part, pair, k).start()
            return carry

        lax.fori_loop(0, count, one, 0)

    def body(acc_a, acc_b):
        load_prev(0, 0).start()

        def first_loads(k, carry):
            load_lhs(0, k).start()
            load_rhs(0, 0, k).start()
            return carry

        lax.fori_loop(0, count, first_loads, 0)
        up_out[0, :, 0:half] = pltpu.matmul_pop(acc_a)
        up_out[0, :, half:WIDE] = pltpu.matmul_pop(acc_b)

        for part in range(2):
            def one_round(pair, carry, part=part):
                buf = lax.rem(pair, 2)

                def push(k):
                    pltpu.matmul_push_rhs(rhs[buf, k, :, 0:half], staging_register=0, mxu_index=0)
                    pltpu.matmul_push_rhs(rhs[buf, k, :, half:WIDE], staging_register=0, mxu_index=1)

                def multiply(k):
                    left = lhs[part, k]
                    pltpu.matmul_acc_lhs(acc_a, left, load_staged_rhs=0)
                    pltpu.matmul_acc_lhs(acc_b, left, load_staged_rhs=0)

                def arrive(k):
                    load_rhs(part, pair, k).wait()

                    @pl.when(pair == 0)
                    def _():
                        load_lhs(part, k).wait()

                arrive(0)

                @pl.when(pair + 1 < rounds)
                def _():
                    fetch(part, pair + 1)

                if part == 0:
                    @pl.when(pair == rounds - 1)
                    def _():
                        fetch(1, 0)

                    @pl.when(pair == 0)
                    def _():
                        def more(k, carry):
                            load_lhs(1, k).start()
                            return carry

                        lax.fori_loop(0, count, more, 0)

                push(0)

                def step(k, carry):
                    arrive(k + 1)
                    multiply(k)
                    push(k + 1)
                    return carry

                lax.fori_loop(0, count - 1, step, 0)
                multiply(count - 1)
                load_prev(part, pair).wait()

                @pl.when(pair >= 2)
                def _():
                    save(part, pair - 2).wait()

                for side, acc in ((0, acc_a), (1, acc_b)):
                    cols = slice(side * half, (side + 1) * half)
                    total = pltpu.matmul_pop(acc) + prev[buf, :, cols]
                    if part == 0:
                        up_out[buf, :, cols] = total
                    else:
                        down_out[buf, cols, :] = total.T
                save(part, pair).start()
                return carry

            lax.fori_loop(0, rounds, one_round, 0)
        for part in range(2):
            for pair in range(rounds - 2, rounds):
                save(part, pair).wait()

    pl.run_scoped(body, pltpu.ACC(0)((width, half), F32), pltpu.ACC(1)((width, half), F32))


def run_weights(nt_all, gt_all, du_all, a_all, acc):
    micro, width, tokens = nt_all.shape
    hidden = du_all.shape[2]
    any_spec = pl.BlockSpec(memory_space=pl.ANY)
    dma = pltpu.SemaphoreType.DMA
    return pl.pallas_call(
        weight_kernel,
        out_shape=(jax.ShapeDtypeStruct((width, hidden), F32), jax.ShapeDtypeStruct((hidden, width), F32)),
        in_specs=[any_spec] * 5,
        out_specs=(any_spec, any_spec),
        scratch_shapes=[
            pltpu.VMEM((2, micro, width, tokens), BF16),
            pltpu.VMEM((2, micro, tokens, WIDE), BF16),
            pltpu.VMEM((2, width, WIDE), F32),
            pltpu.VMEM((2, width, WIDE), F32),
            pltpu.VMEM((2, WIDE, width), F32),
            dma((2, micro)), dma((2, micro)), dma((2,)), dma((2, 2)),
        ],
        compiler_params=pltpu.CompilerParams(vmem_limit_bytes=67043328),
        cost_estimate=pl.CostEstimate(
            flops=4 * micro * tokens * width * hidden, transcendentals=0, bytes_accessed=4 * micro * tokens * hidden),
        name="weights",
    )(nt_all, gt_all, du_all, a_all, acc)


def solution(mesh):
    def device_step(x_in, y_target, w_up, w_down, gain):
        micro, tokens, width = x_in.shape
        nt_all, a_all, du_all, gt_all, _, acc, gain_rows, loss_rows = run_pipeline(x_in, y_target, w_up, w_down, gain)
        grad_up, grad_down = run_weights(nt_all, gt_all, du_all, a_all, acc)
        loss = jnp.sum(loss_rows) * (1.0 / (micro * tokens * width))
        grad_gain = jnp.sum(gain_rows, axis=0, keepdims=True)
        return loss.reshape(1), grad_up[None], grad_down[None], grad_gain

    weight_spec = P("stage", None, None)
    grad_spec = P(("data", "stage"), None, None)
    return jax.shard_map(
        device_step, mesh=mesh,
        in_specs=(P("data", None, None), P("data", None, None), weight_spec, weight_spec, P("stage", None)),
        out_specs=(P("data"), grad_spec, grad_spec, P(("data", "stage"), None)), check_vma=False)
```

```python
import functools

import jax
import jax.numpy as jnp
from jax import lax
from jax.experimental import pallas as pl
from jax.experimental.pallas import tpu as pltpu
from jax.sharding import PartitionSpec as P

MESH = pl.DeviceIdType.MESH
F32 = jnp.float32
BF16 = jnp.bfloat16
NORM_EPS = 1e-6
STAGES = 4
LAG = 3
RING = 13
G_RING = 6
COLS = 256
WCOLS = 512
WIDE = 512
OUTC = 768
BLOCKS = 12
ORDER = (
    [("G", k) for k in range(BLOCKS)] + [(kind, k) for k in range(BLOCKS) for kind in ("N", "E")] + [("B", 0), ("U", 0)]
)
FORWARD_ORDER = (
    [("E", 0)] + [step for k in range(1, BLOCKS) for step in (("E", k), ("A", k - 1))] + [("A", BLOCKS - 1), ("Z", 0)]
)
ROWS = 64
NT = (((1,), (1,)), ((), ()))
GELU_C = 0.7978845608028654
GELU_A = 0.044715


def lag_of(stage):
    return LAG * (STAGES - 1 - stage) + 1 + jnp.where(stage < STAGES // 2, 1, 0)


def pipeline_kernel(x_hbm, y_hbm, w1_hbm, w2_hbm, gain_ref,
                    nt_hbm, a_hbm, du_hbm, gt_hbm, d_hbm, acc_hbm, gg_ref, loss_ref,
                    w1, w2, xring, gring, gsend, nbuf, ntbuf, gtbuf, abuf, dbuf, dubuf, ybuf, acc, wnt, wa, lbuf,
                    wsem, xrecv, grecv, xsem, gsem, ntsem, asem, dosem, dusem, gtsem, disem, ysem, wlsem, accsem,
                    lsend, lrecv, gfree):
    micro, tokens, width = x_hbm.shape
    hidden = w1.shape[1]
    stage = lax.axis_index("stage")
    first = stage == 0
    last = stage == STAGES - 1
    lag = lag_of(stage)
    scale = 1.0 / (micro * tokens * width)

    def at_stage(pos):
        return {"stage": pos}

    def copy_w1():
        return pltpu.make_async_copy(w1_hbm.at[0], w1, wsem.at[0])

    def copy_w2():
        return pltpu.make_async_copy(w2_hbm.at[0], w2, wsem.at[1])

    def load_x(i):
        slot = lax.rem(i, RING)
        return pltpu.make_async_copy(x_hbm.at[i], xring.at[slot], xrecv.at[slot])

    def load_y(i):
        return pltpu.make_async_copy(y_hbm.at[i], ybuf.at[lax.rem(i, 2)], ysem.at[lax.rem(i, 2)])

    def send_x(i):
        return pltpu.make_async_remote_copy(
            src_ref=gring.at[G_RING + lax.rem(i, 2)], dst_ref=xring.at[lax.rem(i, RING)], send_sem=xsem.at[lax.rem(i, 2)],
            recv_sem=xrecv.at[lax.rem(i, RING)], device_id=at_stage(lax.rem(stage + 1, STAGES)), device_id_type=MESH)

    def send_g(i):
        return pltpu.make_async_remote_copy(
            src_ref=gsend.at[lax.rem(i, 2)], dst_ref=gring.at[lax.rem(i, G_RING)], send_sem=gsem.at[lax.rem(i, 2)],
            recv_sem=grecv.at[lax.rem(i, G_RING)], device_id=at_stage(lax.rem(stage + STAGES - 1, STAGES)),
            device_id_type=MESH)

    def save_nt(i):
        return pltpu.make_async_copy(ntbuf.at[lax.rem(i, 2)], nt_hbm.at[i], ntsem.at[lax.rem(i, 2)])

    def save_a(i):
        return pltpu.make_async_copy(abuf.at[lax.rem(i, 2)], a_hbm.at[i], asem.at[lax.rem(i, 2)])

    def save_d(i):
        return pltpu.make_async_copy(dbuf.at[lax.rem(i, 2)], d_hbm.at[i], dosem.at[lax.rem(i, 2)])

    def load_d(i):
        return pltpu.make_async_copy(d_hbm.at[i], dbuf.at[2 + lax.rem(i, 2)], disem.at[lax.rem(i, 2)])

    def save_du(i):
        return pltpu.make_async_copy(dubuf.at[lax.rem(i, 2)], du_hbm.at[i], dusem.at[lax.rem(i, 2)])

    def save_gt(i):
        return pltpu.make_async_copy(gtbuf.at[lax.rem(i, 2)], gt_hbm.at[i], gtsem.at[lax.rem(i, 2)])

    def load_wnt(i):
        return pltpu.make_async_copy(nt_hbm.at[i], wnt, wlsem.at[0])

    def load_wa(i):
        return pltpu.make_async_copy(a_hbm.at[i], wa, wlsem.at[1])

    def save_acc():
        return pltpu.make_async_copy(acc, acc_hbm, accsem)

    copy_w1().start()
    copy_w2().start()

    @pl.when(first)
    def _():
        load_x(0).start()

    load_y(0).start()
    barrier = pltpu.get_barrier_semaphore()
    for step in range(1, STAGES):
        pl.semaphore_signal(barrier, inc=1, device_id=at_stage(lax.rem(stage + step, STAGES)), device_id_type=MESH)
    gg_ref[...] = jnp.zeros_like(gg_ref)
    lbuf[...] = jnp.zeros_like(lbuf)

    def clear(row, carry):
        for part in range(2):
            acc[part, pl.ds(pl.multiple_of(row * 8, 8), 8), :] = jnp.zeros((8, hidden), F32)
        return carry

    lax.fori_loop(0, width // 8, clear, 0)
    pl.semaphore_wait(barrier, STAGES - 1)

    copy_w1().wait()
    copy_w2().wait()

    def normalize(i, slot, two):
        gain = gain_ref[...]
        for row in range(0, tokens, ROWS):
            x_f = xring[slot, row:row + ROWS, :].astype(F32)
            inv = lax.rsqrt(jnp.mean(x_f * x_f, axis=-1, keepdims=True) + NORM_EPS)
            nbuf[row:row + ROWS, :] = (x_f * inv * gain).astype(BF16)
        ntbuf[two] = nbuf[...].T

    def expand(two, col):
        u = jnp.dot(nbuf[...], w1[:, col:col + COLS], preferred_element_type=F32)
        u_sq = u * u
        th = jnp.tanh(u * (GELU_C + (GELU_C * GELU_A) * u_sq))
        h = 0.5 * th + 0.5
        abuf[two, :, col:col + COLS] = (u * h).astype(BF16)
        slope = u * (2.0 * GELU_C + (6.0 * GELU_C * GELU_A) * u_sq)
        dbuf[two, :, col:col + COLS] = h + (h - h * h) * slope

    def finish_forward(slot, two, ocol, update):
        out = (xring[slot, :, ocol].astype(F32) + update).astype(BF16)
        delta = out.astype(F32) - ybuf[two, :, ocol].astype(F32)
        gring[G_RING + two, :, ocol] = jnp.where(last, ((2.0 * scale) * delta).astype(BF16), out)
        lbuf[:, ocol] += jnp.sum((delta * delta).reshape(tokens // 8, 8, -1), axis=0)

    def grad_hidden(g_slot, d_slot, two, col):
        ga = lax.dot_general(gring[g_slot], w2[col:col + COLS, :], NT, preferred_element_type=F32)
        ga = ga.astype(BF16).astype(F32)
        dubuf[two, :, col:col + COLS] = (ga * dbuf[d_slot, :, col:col + COLS]).astype(BF16)

    def finish_backward(slot, g_slot, two, gn_all):
        gsend[two] = gn_all.astype(BF16)
        gain = gain_ref[...]
        for row in range(0, tokens, ROWS):
            x_f = xring[slot, row:row + ROWS, :].astype(F32)
            inv = lax.rsqrt(jnp.mean(x_f * x_f, axis=-1, keepdims=True) + NORM_EPS)
            x_hat = x_f * inv
            gn = gsend[two, row:row + ROWS, :].astype(F32)
            gg_ref[...] += jnp.sum((gn * x_hat).reshape(ROWS // 8, 8, width), axis=0)
            ghat = gn * gain
            gx = inv * (ghat - x_hat * jnp.mean(ghat * x_hat, axis=-1, keepdims=True))
            gsend[two, row:row + ROWS, :] = (gring[g_slot, row:row + ROWS, :].astype(F32) + gx).astype(BF16)

    def compute(do_f, do_b, i, j):
        f_slot, f_two = lax.rem(i, RING), lax.rem(i, 2)
        b_slot, b_two = lax.rem(j, RING), lax.rem(j, 2)
        d_slot = jnp.where(last, b_two, 2 + b_two)
        g_slot = jnp.where(last, G_RING + b_two, lax.rem(j, G_RING))
        blocks = range(hidden // COLS)
        if do_f:
            normalize(i, f_slot, f_two)
        gn_all = None
        update = None
        for kind, k in ORDER if do_b else FORWARD_ORDER:
            if kind == "A":
                part = jnp.dot(abuf[f_two, :, k * COLS:(k + 1) * COLS], w2[k * COLS:(k + 1) * COLS, :],
                               preferred_element_type=F32)
                update = part if update is None else update + part
            if kind == "Z":
                finish_forward(f_slot, f_two, slice(0, width), update)
            if kind == "E" and do_f:
                expand(f_two, k * COLS)
            if kind == "G" and do_b:
                grad_hidden(g_slot, d_slot, b_two, k * COLS)
            if kind == "N" and do_b:
                part = lax.dot_general(dubuf[b_two, :, k * COLS:(k + 1) * COLS], w1[:, k * COLS:(k + 1) * COLS], NT,
                                       preferred_element_type=F32)
                gn_all = part if gn_all is None else gn_all + part
            if kind == "B" and do_b:
                gtbuf[b_two] = gring[g_slot].T
                finish_backward(b_slot, g_slot, b_two, gn_all)
            if kind == "U" and do_f:
                ocol = slice(k * OUTC, (k + 1) * OUTC)
                update = jnp.dot(abuf[f_two], w2[:, ocol], preferred_element_type=F32)
                finish_forward(f_slot, f_two, ocol, update)

    def weight_grads(j):
        two = lax.rem(j, 2)
        load_wnt(j).wait()
        load_wa(j).wait()
        for col in range(0, hidden, WCOLS):
            block = slice(col, col + WCOLS)
            acc[0, :, block] += jnp.dot(wnt[...], dubuf[two, :, block], preferred_element_type=F32)
            acc[1, :, block] += jnp.dot(gtbuf[two], wa[:, block], preferred_element_type=F32)

    def before_forward(i):
        @pl.when(first)
        def _():
            load_x(i).wait()

            @pl.when(i + 1 < micro)
            def _():
                load_x(i + 1).start()

        @pl.when(jnp.logical_not(first))
        def _():
            send_x(i).wait_recv()

        load_y(i).wait()

        @pl.when(i + 1 < micro)
        def _():
            load_y(i + 1).start()

    def after_forward(i):
        save_nt(i).start()
        save_a(i).start()

        @pl.when(jnp.logical_not(last))
        def _():
            save_d(i).start()
            send_x(i).start()

    def before_backward(j):
        @pl.when(jnp.logical_not(last))
        def _():
            load_d(j).wait()
            send_g(j).wait_recv()

    def after_backward(j):
        save_du(j).start()
        save_gt(j).start()

        @pl.when(jnp.logical_not(last) & (j < micro - G_RING))
        def _():
            pl.semaphore_signal(gfree, inc=1, device_id=at_stage(lax.rem(stage + 1, STAGES)), device_id_type=MESH)

        @pl.when(jnp.logical_not(first) & (j >= G_RING))
        def _():
            pl.semaphore_wait(gfree, 1)

        @pl.when(jnp.logical_not(first))
        def _():
            send_g(j).start()

    def tick(t, carry):
        i = t
        j = t - lag
        f_on = i < micro
        b_on = (j >= 0) & (j < micro)

        @pl.when((i >= 2) & (i < micro + 2))
        def _():
            save_nt(i - 2).wait()
            save_a(i - 2).wait()

            @pl.when(jnp.logical_not(last))
            def _():
                save_d(i - 2).wait()
                send_x(i - 2).wait_send()

        @pl.when((j >= 2) & (j < micro + 2))
        def _():
            save_du(j - 2).wait()
            save_gt(j - 2).wait()

            @pl.when(jnp.logical_not(first))
            def _():
                send_g(j - 2).wait_send()

        @pl.when(f_on)
        def _():
            before_forward(i)

        @pl.when(b_on)
        def _():
            before_backward(j)

        @pl.when(jnp.logical_not(last) & (j + 1 >= 0) & (j + 1 < micro))
        def _():
            load_d(j + 1).start()

        w_on = jnp.logical_not(f_on) & (j < micro - 1)

        @pl.when(w_on)
        def _():
            load_wnt(j).start()
            load_wa(j).start()

        @pl.when(j == micro - 1)
        def _():
            save_acc().start()

        @pl.when(f_on & b_on)
        def _():
            compute(True, True, i, j)

        @pl.when(f_on & jnp.logical_not(b_on))
        def _():
            compute(True, False, i, j)

        @pl.when(b_on & jnp.logical_not(f_on))
        def _():
            compute(False, True, i, j)

        @pl.when(b_on)
        def _():
            after_backward(j)

        @pl.when(f_on)
        def _():
            after_forward(i)

        @pl.when(w_on)
        def _():
            weight_grads(j)

        return carry

    lax.fori_loop(0, micro + LAG * (STAGES - 1) + 4, tick, 0)

    save_acc().wait()

    def send_loss(pos):
        return pltpu.make_async_remote_copy(
            src_ref=lbuf, dst_ref=lbuf, send_sem=lsend.at[pos], recv_sem=lrecv, device_id=at_stage(pos),
            device_id_type=MESH)

    @pl.when(last)
    def _():
        for pos in range(STAGES - 1):
            send_loss(pos).start()
        for pos in range(STAGES - 1):
            send_loss(pos).wait_send()

    @pl.when(jnp.logical_not(last))
    def _():
        send_loss(0).wait_recv()

    loss_ref[...] = lbuf[...]


def run_pipeline(x_in, y_target, w_up, w_down, gain):
    micro, tokens, width = x_in.shape
    hidden = w_up.shape[2]
    any_spec = pl.BlockSpec(memory_space=pl.ANY)
    vmem_spec = pl.BlockSpec(memory_space=pltpu.VMEM)
    dma = pltpu.SemaphoreType.DMA
    return pl.pallas_call(
        pipeline_kernel,
        out_shape=(
            jax.ShapeDtypeStruct((micro, width, tokens), BF16),
            jax.ShapeDtypeStruct((micro, tokens, hidden), BF16),
            jax.ShapeDtypeStruct((micro, tokens, hidden), BF16),
            jax.ShapeDtypeStruct((micro, width, tokens), BF16),
            jax.ShapeDtypeStruct((micro, tokens, hidden), F32),
            jax.ShapeDtypeStruct((2, width, hidden), F32),
            jax.ShapeDtypeStruct((8, width), F32),
            jax.ShapeDtypeStruct((8, width), F32),
        ),
        in_specs=[any_spec, any_spec, any_spec, any_spec, vmem_spec],
        out_specs=(any_spec, any_spec, any_spec, any_spec, any_spec, any_spec, vmem_spec, vmem_spec),
        scratch_shapes=[
            pltpu.VMEM((width, hidden), BF16),
            pltpu.VMEM((hidden, width), BF16),
            pltpu.VMEM((RING, tokens, width), BF16),
            pltpu.VMEM((G_RING + 2, tokens, width), BF16),
            pltpu.VMEM((2, tokens, width), BF16),
            pltpu.VMEM((tokens, width), BF16),
            pltpu.VMEM((2, width, tokens), BF16),
            pltpu.VMEM((2, width, tokens), BF16),
            pltpu.VMEM((2, tokens, hidden), BF16),
            pltpu.VMEM((4, tokens, hidden), F32),
            pltpu.VMEM((2, tokens, hidden), BF16),
            pltpu.VMEM((2, tokens, width), BF16),
            pltpu.VMEM((2, width, hidden), F32),
            pltpu.VMEM((width, tokens), BF16),
            pltpu.VMEM((tokens, hidden), BF16),
            pltpu.VMEM((8, width), F32),
            dma((2,)), dma((RING,)), dma((G_RING,)), dma((2,)), dma((2,)), dma((2,)), dma((2,)), dma((2,)), dma((2,)),
            dma((2,)), dma((2,)), dma((2,)), dma((2,)), dma, dma((STAGES - 1,)), dma, pltpu.SemaphoreType.REGULAR,
        ],
        compiler_params=pltpu.CompilerParams(
            collective_id=0, has_side_effects=True,
            vmem_limit_bytes=67043328),
        cost_estimate=pl.CostEstimate(
            flops=8 * micro * tokens * width * hidden, transcendentals=micro * tokens * hidden,
            bytes_accessed=16 * micro * tokens * hidden),
        name="pipeline",
    )(x_in, y_target, w_up, w_down, gain)


def weight_kernel(scale, nt_hbm, gt_hbm, du_hbm, a_hbm, acc_hbm, gg_ref, loss_rows,
                  up_hbm, down_hbm, gain_out, loss_out, lhs, rhs, prev, up_out, down_out, lsem, rsem, psem, osem):
    micro, width, tokens = nt_hbm.shape
    hidden = du_hbm.shape[2]
    rounds = hidden // WIDE
    half = WIDE // 2
    rows = width // 2
    cut = micro - lag_of(lax.axis_index("stage"))
    count = cut + 1

    def source(k):
        return jnp.where(k < cut, k, micro - 1)

    def load_lhs(part, k):
        return pltpu.make_async_copy((nt_hbm, gt_hbm)[part].at[source(k)], lhs.at[part, k], lsem.at[part, k])

    def load_rhs(part, pair, k):
        cols = pl.ds(pl.multiple_of(pair * WIDE, WIDE), WIDE)
        buf = lax.rem(pair, 2)
        return pltpu.make_async_copy((du_hbm, a_hbm)[part].at[source(k), :, cols], rhs.at[buf, k], rsem.at[buf, k])

    def load_prev(part, pair):
        cols = pl.ds(pl.multiple_of(pair * WIDE, WIDE), WIDE)
        buf = lax.rem(pair, 2)
        return pltpu.make_async_copy(acc_hbm.at[part, :, cols], prev.at[buf], psem.at[buf])

    def save(part, pair):
        start = pl.multiple_of(pair * WIDE, WIDE)
        buf = lax.rem(pair, 2)
        if part == 0:
            return pltpu.make_async_copy(up_out.at[buf], up_hbm.at[:, pl.ds(start, WIDE)], osem.at[0, buf])
        return pltpu.make_async_copy(down_out.at[buf], down_hbm.at[pl.ds(start, WIDE), :], osem.at[1, buf])

    def fetch(part, pair):
        load_prev(part, pair).start()

        def one(k, carry):
            load_rhs(part, pair, k).start()
            return carry

        lax.fori_loop(0, count, one, 0)

    def body(top_a, top_b, low_a, low_b):
        def first_loads(k, carry):
            load_lhs(0, k).start()
            load_rhs(0, 0, k).start()
            return carry

        lax.fori_loop(0, count, first_loads, 0)
        load_prev(0, 0).start()
        gain_out[...] = jnp.sum(gg_ref[...], axis=0, keepdims=True)
        loss_out[0] = jnp.sum(loss_rows[...]) * scale

        def drain(part, buf, low):
            first_row = rows if low else 0
            for side, acc in enumerate((low_a, low_b) if low else (top_a, top_b)):
                cols = slice(side * half, (side + 1) * half)
                total = pltpu.matmul_pop(acc) + prev[buf, first_row:first_row + rows, cols]
                if part == 0:
                    up_out[buf, first_row:first_row + rows, cols] = total
                else:
                    down_out[buf, cols, first_row:first_row + rows] = total.T

        for low in range(2):
            for side, acc in enumerate((low_a, low_b) if low else (top_a, top_b)):
                up_out[1, low * rows:(low + 1) * rows, side * half:(side + 1) * half] = pltpu.matmul_pop(acc)

        def finish_low(part, pair):
            drain(part, lax.rem(pair, 2), True)
            save(part, pair).start()

        for part in range(2):
            def one_round(pair, carry, part=part):
                buf = lax.rem(pair, 2)

                def push(k):
                    pltpu.matmul_push_rhs(rhs[buf, k, :, 0:half], staging_register=0, mxu_index=0)
                    pltpu.matmul_push_rhs(rhs[buf, k, :, half:WIDE], staging_register=0, mxu_index=1)

                def multiply(k, low):
                    left = lhs[part, k, rows:width, :] if low else lhs[part, k, 0:rows, :]
                    pltpu.matmul_acc_lhs(low_a if low else top_a, left, load_staged_rhs=0)
                    pltpu.matmul_acc_lhs(low_b if low else top_b, left, load_staged_rhs=0)

                def arrive(k):
                    load_rhs(part, pair, k).wait()

                    @pl.when(pair == 0)
                    def _():
                        load_lhs(part, k).wait()

                def step_top(k, carry):
                    arrive(k + 1)
                    multiply(k, False)
                    push(k + 1)
                    return carry

                def step_low(k, carry):
                    multiply(k, True)
                    push(k + 1)
                    return carry

                arrive(0)
                arrive(1)
                push(0)
                if part == 0:
                    @pl.when(pair == 0)
                    def _():
                        multiply(0, False)
                        push(1)

                    @pl.when(pair > 0)
                    def _():
                        multiply(0, False)
                        push(1)
                        drain(0, 1 - buf, True)
                        save(0, pair - 1).start()
                else:
                    @pl.when(pair == 0)
                    def _():
                        multiply(0, False)
                        push(1)
                        drain(0, (rounds - 1) % 2, True)
                        save(0, rounds - 1).start()

                    @pl.when(pair > 0)
                    def _():
                        multiply(0, False)
                        push(1)
                        drain(1, 1 - buf, True)
                        save(1, pair - 1).start()

                @pl.when(pair + 1 < rounds)
                def _():
                    fetch(part, pair + 1)

                if part == 0:
                    @pl.when(pair == rounds - 1)
                    def _():
                        fetch(1, 0)

                    @pl.when(pair == 0)
                    def _():
                        def more(k, carry):
                            load_lhs(1, k).start()
                            return carry

                        lax.fori_loop(0, count, more, 0)

                lax.fori_loop(1, count - 1, step_top, 0)
                load_prev(part, pair).wait()

                @pl.when(pair >= 2)
                def _():
                    save(part, pair - 2).wait()

                multiply(count - 1, False)
                push(0)
                multiply(0, True)
                push(1)
                drain(part, buf, False)
                lax.fori_loop(1, count - 1, step_low, 0)
                multiply(count - 1, True)
                return carry

            lax.fori_loop(0, rounds, one_round, 0)
        drain(1, (rounds - 1) % 2, True)
        save(1, rounds - 1).start()
        for part in range(2):
            for pair in range(rounds - 2, rounds):
                save(part, pair).wait()

    top, low = (width // 2, half), (width // 2, half)
    pl.run_scoped(body, pltpu.ACC(0)(top, F32), pltpu.ACC(1)(top, F32), pltpu.ACC(0)(low, F32), pltpu.ACC(1)(low, F32))


def run_weights(nt_all, gt_all, du_all, a_all, acc, gain_rows, loss_rows):
    micro, width, tokens = nt_all.shape
    hidden = du_all.shape[2]
    any_spec = pl.BlockSpec(memory_space=pl.ANY)
    vmem_spec = pl.BlockSpec(memory_space=pltpu.VMEM)
    dma = pltpu.SemaphoreType.DMA
    return pl.pallas_call(
        functools.partial(weight_kernel, 1.0 / (micro * tokens * width)),
        out_shape=(
            jax.ShapeDtypeStruct((width, hidden), F32),
            jax.ShapeDtypeStruct((hidden, width), F32),
            jax.ShapeDtypeStruct((1, width), F32),
            jax.ShapeDtypeStruct((1,), F32),
        ),
        in_specs=[any_spec] * 5 + [vmem_spec] * 2,
        out_specs=(any_spec, any_spec, vmem_spec, pl.BlockSpec(memory_space=pltpu.SMEM)),
        scratch_shapes=[
            pltpu.VMEM((2, micro, width, tokens), BF16),
            pltpu.VMEM((2, micro, tokens, WIDE), BF16),
            pltpu.VMEM((2, width, WIDE), F32),
            pltpu.VMEM((2, width, WIDE), F32),
            pltpu.VMEM((2, WIDE, width), F32),
            dma((2, micro)), dma((2, micro)), dma((2,)), dma((2, 2)),
        ],
        compiler_params=pltpu.CompilerParams(vmem_limit_bytes=67043328),
        cost_estimate=pl.CostEstimate(
            flops=4 * micro * tokens * width * hidden, transcendentals=0, bytes_accessed=4 * micro * tokens * hidden),
        name="weights",
    )(nt_all, gt_all, du_all, a_all, acc, gain_rows, loss_rows)


def solution(mesh):
    def device_step(x_in, y_target, w_up, w_down, gain):
        nt_all, a_all, du_all, gt_all, _, acc, gain_rows, loss_rows = run_pipeline(x_in, y_target, w_up, w_down, gain)
        grad_up, grad_down, grad_gain, loss = run_weights(nt_all, gt_all, du_all, a_all, acc, gain_rows, loss_rows)
        return loss, grad_up[None], grad_down[None], grad_gain

    weight_spec = P("stage", None, None)
    grad_spec = P(("data", "stage"), None, None)
    return jax.shard_map(
        device_step, mesh=mesh,
        in_specs=(P("data", None, None), P("data", None, None), weight_spec, weight_spec, P("stage", None)),
        out_specs=(P("data"), grad_spec, grad_spec, P(("data", "stage"), None)), check_vma=False)
```

```python
import functools

import jax
import jax.numpy as jnp
from jax import lax
from jax.experimental import pallas as pl
from jax.experimental.pallas import tpu as pltpu
from jax.sharding import PartitionSpec as P

MESH = pl.DeviceIdType.MESH
F32 = jnp.float32
BF16 = jnp.bfloat16
NORM_EPS = 1e-6
STAGES = 4
LAGS = (13, 10, 5, 1)
RING = 15
G_RING = 6
COLS = 256
WCOLS = 512
WIDE = 512
OUTC = 768
BLOCKS = 12
ORDER = (
    [("G", k) for k in range(BLOCKS)] + [(kind, k) for k in range(BLOCKS) for kind in ("N", "E")] + [("B", 0), ("U", 0)]
)
FORWARD_ORDER = (
    [("E", 0)] + [step for k in range(1, BLOCKS) for step in (("E", k), ("A", k - 1))] + [("A", BLOCKS - 1), ("Z", 0)]
)
ROWS = 64
NT = (((1,), (1,)), ((), ()))
GELU_C = 0.7978845608028654
GELU_A = 0.044715


def lag_of(stage):
    lag = LAGS[0]
    for pos in range(1, STAGES):
        lag = jnp.where(stage == pos, LAGS[pos], lag)
    return lag


def pipeline_kernel(x_hbm, y_hbm, w1_hbm, w2_hbm, gain_ref,
                    nt_hbm, a_hbm, du_hbm, gt_hbm, d_hbm, acc_hbm, gg_ref, loss_ref,
                    w1, w2, xring, gring, gsend, nbuf, ntbuf, gtbuf, abuf, dbuf, dubuf, ybuf, acc, wnt, wa, lbuf,
                    wsem, xrecv, grecv, xsem, gsem, ntsem, asem, dosem, dusem, gtsem, disem, ysem, wlsem, accsem,
                    lsend, lrecv, gfree):
    micro, tokens, width = x_hbm.shape
    hidden = w1.shape[1]
    stage = lax.axis_index("stage")
    first = stage == 0
    last = stage == STAGES - 1
    lag = lag_of(stage)
    scale = 1.0 / (micro * tokens * width)

    def at_stage(pos):
        return {"stage": pos}

    def copy_w1():
        return pltpu.make_async_copy(w1_hbm.at[0], w1, wsem.at[0])

    def copy_w2():
        return pltpu.make_async_copy(w2_hbm.at[0], w2, wsem.at[1])

    def load_x(i):
        slot = lax.rem(i, RING)
        return pltpu.make_async_copy(x_hbm.at[i], xring.at[slot], xrecv.at[slot])

    def load_y(i):
        return pltpu.make_async_copy(y_hbm.at[i], ybuf.at[lax.rem(i, 2)], ysem.at[lax.rem(i, 2)])

    def send_x(i):
        return pltpu.make_async_remote_copy(
            src_ref=gring.at[G_RING + lax.rem(i, 2)], dst_ref=xring.at[lax.rem(i, RING)], send_sem=xsem.at[lax.rem(i, 2)],
            recv_sem=xrecv.at[lax.rem(i, RING)], device_id=at_stage(lax.rem(stage + 1, STAGES)), device_id_type=MESH)

    def send_g(i):
        return pltpu.make_async_remote_copy(
            src_ref=gsend.at[lax.rem(i, 2)], dst_ref=gring.at[lax.rem(i, G_RING)], send_sem=gsem.at[lax.rem(i, 2)],
            recv_sem=grecv.at[lax.rem(i, G_RING)], device_id=at_stage(lax.rem(stage + STAGES - 1, STAGES)),
            device_id_type=MESH)

    def save_nt(i):
        return pltpu.make_async_copy(ntbuf.at[lax.rem(i, 2)], nt_hbm.at[i], ntsem.at[lax.rem(i, 2)])

    def save_a(i):
        return pltpu.make_async_copy(abuf.at[lax.rem(i, 2)], a_hbm.at[i], asem.at[lax.rem(i, 2)])

    def save_d(i):
        return pltpu.make_async_copy(dbuf.at[lax.rem(i, 2)], d_hbm.at[i], dosem.at[lax.rem(i, 2)])

    def load_d(i):
        return pltpu.make_async_copy(d_hbm.at[i], dbuf.at[2 + lax.rem(i, 2)], disem.at[lax.rem(i, 2)])

    def save_du(i):
        return pltpu.make_async_copy(dubuf.at[lax.rem(i, 2)], du_hbm.at[i], dusem.at[lax.rem(i, 2)])

    def save_gt(i):
        return pltpu.make_async_copy(gtbuf.at[lax.rem(i, 2)], gt_hbm.at[i], gtsem.at[lax.rem(i, 2)])

    def load_wnt(i):
        return pltpu.make_async_copy(nt_hbm.at[i], wnt, wlsem.at[0])

    def load_wa(i):
        return pltpu.make_async_copy(a_hbm.at[i], wa, wlsem.at[1])

    def save_acc():
        return pltpu.make_async_copy(acc, acc_hbm, accsem)

    copy_w1().start()
    copy_w2().start()

    @pl.when(first)
    def _():
        load_x(0).start()

    load_y(0).start()
    barrier = pltpu.get_barrier_semaphore()
    for step in range(1, STAGES):
        pl.semaphore_signal(barrier, inc=1, device_id=at_stage(lax.rem(stage + step, STAGES)), device_id_type=MESH)
    gg_ref[...] = jnp.zeros_like(gg_ref)
    lbuf[...] = jnp.zeros_like(lbuf)

    def clear(row, carry):
        for part in range(2):
            acc[part, pl.ds(pl.multiple_of(row * 8, 8), 8), :] = jnp.zeros((8, hidden), F32)
        return carry

    lax.fori_loop(0, width // 8, clear, 0)
    pl.semaphore_wait(barrier, STAGES - 1)

    copy_w1().wait()
    copy_w2().wait()

    def normalize(i, slot, two):
        gain = gain_ref[...]
        for row in range(0, tokens, ROWS):
            x_f = xring[slot, row:row + ROWS, :].astype(F32)
            inv = lax.rsqrt(jnp.mean(x_f * x_f, axis=-1, keepdims=True) + NORM_EPS)
            nbuf[row:row + ROWS, :] = (x_f * inv * gain).astype(BF16)
        ntbuf[two] = nbuf[...].T

    def expand(two, col):
        u = jnp.dot(nbuf[...], w1[:, col:col + COLS], preferred_element_type=F32)
        u_sq = u * u
        th = jnp.tanh(u * (GELU_C + (GELU_C * GELU_A) * u_sq))
        h = 0.5 * th + 0.5
        abuf[two, :, col:col + COLS] = (u * h).astype(BF16)
        slope = u * (2.0 * GELU_C + (6.0 * GELU_C * GELU_A) * u_sq)
        dbuf[two, :, col:col + COLS] = h + (h - h * h) * slope

    def finish_forward(slot, two, ocol, update):
        out = (xring[slot, :, ocol].astype(F32) + update).astype(BF16)
        delta = out.astype(F32) - ybuf[two, :, ocol].astype(F32)
        gring[G_RING + two, :, ocol] = jnp.where(last, ((2.0 * scale) * delta).astype(BF16), out)
        lbuf[:, ocol] += jnp.sum((delta * delta).reshape(tokens // 8, 8, -1), axis=0)

    def grad_hidden(g_slot, d_slot, two, col):
        ga = lax.dot_general(gring[g_slot], w2[col:col + COLS, :], NT, preferred_element_type=F32)
        ga = ga.astype(BF16).astype(F32)
        dubuf[two, :, col:col + COLS] = (ga * dbuf[d_slot, :, col:col + COLS]).astype(BF16)

    def finish_backward(slot, g_slot, two, gn_all):
        gsend[two] = gn_all.astype(BF16)
        gain = gain_ref[...]
        for row in range(0, tokens, ROWS):
            x_f = xring[slot, row:row + ROWS, :].astype(F32)
            inv = lax.rsqrt(jnp.mean(x_f * x_f, axis=-1, keepdims=True) + NORM_EPS)
            x_hat = x_f * inv
            gn = gsend[two, row:row + ROWS, :].astype(F32)
            gg_ref[...] += jnp.sum((gn * x_hat).reshape(ROWS // 8, 8, width), axis=0)
            ghat = gn * gain
            gx = inv * (ghat - x_hat * jnp.mean(ghat * x_hat, axis=-1, keepdims=True))
            gsend[two, row:row + ROWS, :] = (gring[g_slot, row:row + ROWS, :].astype(F32) + gx).astype(BF16)

    def compute(do_f, do_b, i, j):
        f_slot, f_two = lax.rem(i, RING), lax.rem(i, 2)
        b_slot, b_two = lax.rem(j, RING), lax.rem(j, 2)
        d_slot = jnp.where(last, b_two, 2 + b_two)
        g_slot = jnp.where(last, G_RING + b_two, lax.rem(j, G_RING))
        blocks = range(hidden // COLS)
        if do_f:
            normalize(i, f_slot, f_two)
        gn_all = None
        update = None
        for kind, k in ORDER if do_b else FORWARD_ORDER:
            if kind == "A":
                part = jnp.dot(abuf[f_two, :, k * COLS:(k + 1) * COLS], w2[k * COLS:(k + 1) * COLS, :],
                               preferred_element_type=F32)
                update = part if update is None else update + part
            if kind == "Z":
                finish_forward(f_slot, f_two, slice(0, width), update)
            if kind == "E" and do_f:
                expand(f_two, k * COLS)
            if kind == "G" and do_b:
                grad_hidden(g_slot, d_slot, b_two, k * COLS)
            if kind == "N" and do_b:
                part = lax.dot_general(dubuf[b_two, :, k * COLS:(k + 1) * COLS], w1[:, k * COLS:(k + 1) * COLS], NT,
                                       preferred_element_type=F32)
                gn_all = part if gn_all is None else gn_all + part
            if kind == "B" and do_b:
                gtbuf[b_two] = gring[g_slot].T
                finish_backward(b_slot, g_slot, b_two, gn_all)
            if kind == "U" and do_f:
                ocol = slice(k * OUTC, (k + 1) * OUTC)
                update = jnp.dot(abuf[f_two], w2[:, ocol], preferred_element_type=F32)
                finish_forward(f_slot, f_two, ocol, update)

    def weight_grads(j):
        two = lax.rem(j, 2)
        load_wnt(j).wait()
        load_wa(j).wait()
        for col in range(0, hidden, WCOLS):
            block = slice(col, col + WCOLS)
            acc[0, :, block] += jnp.dot(wnt[...], dubuf[two, :, block], preferred_element_type=F32)
            acc[1, :, block] += jnp.dot(gtbuf[two], wa[:, block], preferred_element_type=F32)

    def before_forward(i):
        @pl.when(first)
        def _():
            load_x(i).wait()

            @pl.when(i + 1 < micro)
            def _():
                load_x(i + 1).start()

        @pl.when(jnp.logical_not(first))
        def _():
            send_x(i).wait_recv()

        load_y(i).wait()

        @pl.when(i + 1 < micro)
        def _():
            load_y(i + 1).start()

    def after_forward(i):
        save_nt(i).start()
        save_a(i).start()

        @pl.when(jnp.logical_not(last))
        def _():
            save_d(i).start()
            send_x(i).start()

    def before_backward(j):
        @pl.when(jnp.logical_not(last))
        def _():
            load_d(j).wait()
            send_g(j).wait_recv()

    def after_backward(j):
        save_du(j).start()
        save_gt(j).start()

        @pl.when(jnp.logical_not(last) & (j < micro - G_RING))
        def _():
            pl.semaphore_signal(gfree, inc=1, device_id=at_stage(lax.rem(stage + 1, STAGES)), device_id_type=MESH)

        @pl.when(jnp.logical_not(first) & (j >= G_RING))
        def _():
            pl.semaphore_wait(gfree, 1)

        @pl.when(jnp.logical_not(first))
        def _():
            send_g(j).start()

    def tick(t, carry):
        i = t
        j = t - lag
        f_on = i < micro
        b_on = (j >= 0) & (j < micro)

        @pl.when((i >= 2) & (i < micro + 2))
        def _():
            save_nt(i - 2).wait()
            save_a(i - 2).wait()

            @pl.when(jnp.logical_not(last))
            def _():
                save_d(i - 2).wait()
                send_x(i - 2).wait_send()

        @pl.when((j >= 2) & (j < micro + 2))
        def _():
            save_du(j - 2).wait()
            save_gt(j - 2).wait()

            @pl.when(jnp.logical_not(first))
            def _():
                send_g(j - 2).wait_send()

        @pl.when(f_on)
        def _():
            before_forward(i)

        @pl.when(b_on)
        def _():
            before_backward(j)

        @pl.when(jnp.logical_not(last) & (j + 1 >= 0) & (j + 1 < micro))
        def _():
            load_d(j + 1).start()

        w_on = jnp.logical_not(f_on) & (j < micro - 1)

        @pl.when(w_on)
        def _():
            load_wnt(j).start()
            load_wa(j).start()

        @pl.when(jnp.logical_not(last) & (j == micro - 1))
        def _():
            save_acc().start()

        @pl.when(f_on & b_on)
        def _():
            compute(True, True, i, j)

        @pl.when(f_on & jnp.logical_not(b_on))
        def _():
            compute(True, False, i, j)

        @pl.when(b_on & jnp.logical_not(f_on))
        def _():
            compute(False, True, i, j)

        @pl.when(b_on)
        def _():
            after_backward(j)

        @pl.when(f_on)
        def _():
            after_forward(i)

        @pl.when(w_on)
        def _():
            weight_grads(j)

        return carry

    lax.fori_loop(0, micro + LAGS[0] + 2, tick, 0)

    @pl.when(jnp.logical_not(last))
    def _():
        save_acc().wait()

    def send_loss(pos):
        return pltpu.make_async_remote_copy(
            src_ref=lbuf, dst_ref=lbuf, send_sem=lsend.at[pos], recv_sem=lrecv, device_id=at_stage(pos),
            device_id_type=MESH)

    @pl.when(last)
    def _():
        for pos in range(STAGES - 1):
            send_loss(pos).start()
        for pos in range(STAGES - 1):
            send_loss(pos).wait_send()

    @pl.when(jnp.logical_not(last))
    def _():
        send_loss(0).wait_recv()

    loss_ref[...] = lbuf[...]


def run_pipeline(x_in, y_target, w_up, w_down, gain):
    micro, tokens, width = x_in.shape
    hidden = w_up.shape[2]
    any_spec = pl.BlockSpec(memory_space=pl.ANY)
    vmem_spec = pl.BlockSpec(memory_space=pltpu.VMEM)
    dma = pltpu.SemaphoreType.DMA
    return pl.pallas_call(
        pipeline_kernel,
        out_shape=(
            jax.ShapeDtypeStruct((micro, width, tokens), BF16),
            jax.ShapeDtypeStruct((micro, tokens, hidden), BF16),
            jax.ShapeDtypeStruct((micro, tokens, hidden), BF16),
            jax.ShapeDtypeStruct((micro, width, tokens), BF16),
            jax.ShapeDtypeStruct((micro, tokens, hidden), F32),
            jax.ShapeDtypeStruct((2, width, hidden), F32),
            jax.ShapeDtypeStruct((8, width), F32),
            jax.ShapeDtypeStruct((8, width), F32),
        ),
        in_specs=[any_spec, any_spec, any_spec, any_spec, vmem_spec],
        out_specs=(any_spec, any_spec, any_spec, any_spec, any_spec, any_spec, vmem_spec, vmem_spec),
        scratch_shapes=[
            pltpu.VMEM((width, hidden), BF16),
            pltpu.VMEM((hidden, width), BF16),
            pltpu.VMEM((RING, tokens, width), BF16),
            pltpu.VMEM((G_RING + 2, tokens, width), BF16),
            pltpu.VMEM((2, tokens, width), BF16),
            pltpu.VMEM((tokens, width), BF16),
            pltpu.VMEM((2, width, tokens), BF16),
            pltpu.VMEM((2, width, tokens), BF16),
            pltpu.VMEM((2, tokens, hidden), BF16),
            pltpu.VMEM((4, tokens, hidden), F32),
            pltpu.VMEM((2, tokens, hidden), BF16),
            pltpu.VMEM((2, tokens, width), BF16),
            pltpu.VMEM((2, width, hidden), F32),
            pltpu.VMEM((width, tokens), BF16),
            pltpu.VMEM((tokens, hidden), BF16),
            pltpu.VMEM((8, width), F32),
            dma((2,)), dma((RING,)), dma((G_RING,)), dma((2,)), dma((2,)), dma((2,)), dma((2,)), dma((2,)), dma((2,)),
            dma((2,)), dma((2,)), dma((2,)), dma((2,)), dma, dma((STAGES - 1,)), dma, pltpu.SemaphoreType.REGULAR,
        ],
        compiler_params=pltpu.CompilerParams(
            collective_id=0, has_side_effects=True,
            vmem_limit_bytes=67043328),
        cost_estimate=pl.CostEstimate(
            flops=8 * micro * tokens * width * hidden, transcendentals=micro * tokens * hidden,
            bytes_accessed=16 * micro * tokens * hidden),
        name="pipeline",
    )(x_in, y_target, w_up, w_down, gain)


def weight_kernel(scale, nt_hbm, gt_hbm, du_hbm, a_hbm, acc_hbm, gg_ref, loss_rows,
                  up_hbm, down_hbm, gain_out, loss_out, lhs, rhs, prev, up_out, down_out, lsem, rsem, psem, osem):
    micro, width, tokens = nt_hbm.shape
    hidden = du_hbm.shape[2]
    rounds = hidden // WIDE
    half = WIDE // 2
    rows = width // 2
    lag = lag_of(lax.axis_index("stage"))
    has_prev = lag > 1
    cut = micro - lag
    count = cut + 1

    def source(k):
        return jnp.where(k < cut, k, micro - 1)

    def load_lhs(part, k):
        return pltpu.make_async_copy((nt_hbm, gt_hbm)[part].at[source(k)], lhs.at[part, k], lsem.at[part, k])

    def load_rhs(part, pair, k):
        cols = pl.ds(pl.multiple_of(pair * WIDE, WIDE), WIDE)
        buf = lax.rem(pair, 2)
        return pltpu.make_async_copy((du_hbm, a_hbm)[part].at[source(k), :, cols], rhs.at[buf, k], rsem.at[buf, k])

    def load_prev(part, pair):
        cols = pl.ds(pl.multiple_of(pair * WIDE, WIDE), WIDE)
        buf = lax.rem(pair, 2)
        return pltpu.make_async_copy(acc_hbm.at[part, :, cols], prev.at[buf], psem.at[buf])

    def save(part, pair):
        start = pl.multiple_of(pair * WIDE, WIDE)
        buf = lax.rem(pair, 2)
        if part == 0:
            return pltpu.make_async_copy(up_out.at[buf], up_hbm.at[:, pl.ds(start, WIDE)], osem.at[0, buf])
        return pltpu.make_async_copy(down_out.at[buf], down_hbm.at[pl.ds(start, WIDE), :], osem.at[1, buf])

    def fetch(part, pair):
        load_prev(part, pair).start()

        def one(k, carry):
            load_rhs(part, pair, k).start()
            return carry

        lax.fori_loop(0, count, one, 0)

    def body(top_a, top_b, low_a, low_b):
        tops, lows = (top_a, top_b), (low_a, low_b)

        def first_loads(k, carry):
            load_lhs(0, k).start()
            load_rhs(0, 0, k).start()
            return carry

        lax.fori_loop(0, count, first_loads, 0)
        load_prev(0, 0).start()
        gain_out[...] = jnp.sum(gg_ref[...], axis=0, keepdims=True)
        loss_out[0] = jnp.sum(loss_rows[...]) * scale
        for accs, first_row in ((tops, 0), (lows, rows)):
            for side, acc in enumerate(accs):
                up_out[1, first_row:first_row + rows, side * half:(side + 1) * half] = pltpu.matmul_pop(acc)

        def drain(part, buf, low):
            first_row = rows if low else 0
            for side, acc in enumerate(lows if low else tops):
                cols = slice(side * half, (side + 1) * half)
                before = jnp.where(has_prev, prev[buf, first_row:first_row + rows, cols], 0.0)
                total = pltpu.matmul_pop(acc) + before
                if part == 0:
                    up_out[buf, first_row:first_row + rows, cols] = total
                else:
                    down_out[buf, cols, first_row:first_row + rows] = total.T

        def push(buf, k):
            pltpu.matmul_push_rhs(rhs[buf, k, :, 0:half], staging_register=0, mxu_index=0)
            pltpu.matmul_push_rhs(rhs[buf, k, :, half:WIDE], staging_register=0, mxu_index=1)

        def multiply_top(part, k):
            left = lhs[part, k, 0:rows, :]
            for acc in tops:
                pltpu.matmul_acc_lhs(acc, left, load_staged_rhs=0)

        def multiply_low(part, k):
            left = lhs[part, k, rows:width, :]
            for acc in lows:
                pltpu.matmul_acc_lhs(acc, left)

        for part in range(2):
            def one_round(pair, carry, part=part):
                buf = lax.rem(pair, 2)

                def arrive(k):
                    load_rhs(part, pair, k).wait()

                    @pl.when(pair == 0)
                    def _():
                        load_lhs(part, k).wait()

                def start_round(drain_part, drain_buf):
                    multiply_top(part, 0)
                    if drain_part is not None:
                        drain(drain_part, drain_buf, True)
                    push(buf, 1)
                    multiply_low(part, 0)

                def step(k):
                    multiply_top(part, k)
                    push(buf, k + 1)
                    multiply_low(part, k)

                def two_steps(i, carry):
                    k = 1 + 2 * i
                    arrive(k + 1)
                    arrive(k + 2)
                    step(k)
                    step(k + 1)
                    return carry

                arrive(0)
                arrive(1)

                push(buf, 0)

                @pl.when(pair == 0)
                def _():
                    if part == 0:
                        start_round(None, None)
                    else:
                        start_round(0, (rounds - 1) % 2)
                        save(0, rounds - 1).start()

                @pl.when(pair > 0)
                def _():
                    start_round(part, 1 - buf)
                    save(part, pair - 1).start()

                @pl.when(pair + 1 < rounds)
                def _():
                    fetch(part, pair + 1)

                if part == 0:
                    @pl.when(pair == rounds - 1)
                    def _():
                        fetch(1, 0)

                    @pl.when(pair == 0)
                    def _():
                        def more(k, carry):
                            load_lhs(1, k).start()
                            return carry

                        lax.fori_loop(0, count, more, 0)

                lax.fori_loop(0, (count - 2) // 2, two_steps, 0)

                @pl.when(lax.rem(count, 2) == 1)
                def _():
                    arrive(count - 1)
                    step(count - 2)

                load_prev(part, pair).wait()

                @pl.when(pair >= 2)
                def _():
                    save(part, pair - 2).wait()

                multiply_top(part, count - 1)
                multiply_low(part, count - 1)
                drain(part, buf, False)
                return carry

            lax.fori_loop(0, rounds, one_round, 0)
        drain(1, (rounds - 1) % 2, True)
        save(1, rounds - 1).start()
        for part in range(2):
            for pair in range(rounds - 2, rounds):
                save(part, pair).wait()

    shape = (rows, half)
    pl.run_scoped(
        body, pltpu.ACC(0)(shape, F32), pltpu.ACC(1)(shape, F32), pltpu.ACC(0)(shape, F32), pltpu.ACC(1)(shape, F32))


def run_weights(nt_all, gt_all, du_all, a_all, acc, gain_rows, loss_rows):
    micro, width, tokens = nt_all.shape
    hidden = du_all.shape[2]
    any_spec = pl.BlockSpec(memory_space=pl.ANY)
    vmem_spec = pl.BlockSpec(memory_space=pltpu.VMEM)
    dma = pltpu.SemaphoreType.DMA
    return pl.pallas_call(
        functools.partial(weight_kernel, 1.0 / (micro * tokens * width)),
        out_shape=(
            jax.ShapeDtypeStruct((width, hidden), F32),
            jax.ShapeDtypeStruct((hidden, width), F32),
            jax.ShapeDtypeStruct((1, width), F32),
            jax.ShapeDtypeStruct((1,), F32),
        ),
        in_specs=[any_spec] * 5 + [vmem_spec] * 2,
        out_specs=(any_spec, any_spec, vmem_spec, pl.BlockSpec(memory_space=pltpu.SMEM)),
        scratch_shapes=[
            pltpu.VMEM((2, micro, width, tokens), BF16),
            pltpu.VMEM((2, micro, tokens, WIDE), BF16),
            pltpu.VMEM((2, width, WIDE), F32),
            pltpu.VMEM((2, width, WIDE), F32),
            pltpu.VMEM((2, WIDE, width), F32),
            dma((2, micro)), dma((2, micro)), dma((2,)), dma((2, 2)),
        ],
        compiler_params=pltpu.CompilerParams(vmem_limit_bytes=67043328),
        cost_estimate=pl.CostEstimate(
            flops=4 * micro * tokens * width * hidden, transcendentals=0, bytes_accessed=4 * micro * tokens * hidden),
        name="weights",
    )(nt_all, gt_all, du_all, a_all, acc, gain_rows, loss_rows)


def solution(mesh):
    def device_step(x_in, y_target, w_up, w_down, gain):
        nt_all, a_all, du_all, gt_all, _, acc, gain_rows, loss_rows = run_pipeline(x_in, y_target, w_up, w_down, gain)
        grad_up, grad_down, grad_gain, loss = run_weights(nt_all, gt_all, du_all, a_all, acc, gain_rows, loss_rows)
        return loss, grad_up[None], grad_down[None], grad_gain

    weight_spec = P("stage", None, None)
    grad_spec = P(("data", "stage"), None, None)
    return jax.shard_map(
        device_step, mesh=mesh,
        in_specs=(P("data", None, None), P("data", None, None), weight_spec, weight_spec, P("stage", None)),
        out_specs=(P("data"), grad_spec, grad_spec, P(("data", "stage"), None)), check_vma=False)
```

```python
import functools

import jax
import jax.numpy as jnp
from jax import lax
from jax.experimental import pallas as pl
from jax.experimental.pallas import tpu as pltpu
from jax.sharding import PartitionSpec as P

MESH = pl.DeviceIdType.MESH
F32 = jnp.float32
BF16 = jnp.bfloat16
NORM_EPS = 1e-6
STAGES = 4
LAGS = (13, 10, 4, 1)
SKIP = 2
RING = 15
G_RING = 6
COLS = 256
WCOLS = 512
WIDE = 512
OUTC = 768
BLOCKS = 12
ORDER = (
    [("G", k) for k in range(BLOCKS)] + [(kind, k) for k in range(BLOCKS) for kind in ("N", "E")] + [("B", 0), ("U", 0)]
)
FORWARD_ORDER = (
    [("E", 0)] + [step for k in range(1, BLOCKS) for step in (("E", k), ("A", k - 1))] + [("A", BLOCKS - 1), ("Z", 0)]
)
ROWS = 64
NT = (((1,), (1,)), ((), ()))
GELU_C = 0.7978845608028654
GELU_A = 0.044715


def lag_of(stage):
    lag = LAGS[0]
    for pos in range(1, STAGES):
        lag = jnp.where(stage == pos, LAGS[pos], lag)
    return lag


def pipeline_kernel(x_hbm, y_hbm, w1_hbm, w2_hbm, gain_ref,
                    nt_hbm, a_hbm, du_hbm, gt_hbm, d_hbm, acc_hbm, gg_ref, loss_ref,
                    w1, w2, xring, gring, gsend, nbuf, ntbuf, gtbuf, abuf, dbuf, dubuf, ybuf, acc, wnt, wa, lbuf,
                    wsem, xrecv, grecv, xsem, gsem, ntsem, asem, dosem, dusem, gtsem, disem, ysem, wlsem, accsem,
                    lsend, lrecv, gfree):
    micro, tokens, width = x_hbm.shape
    hidden = w1.shape[1]
    stage = lax.axis_index("stage")
    first = stage == 0
    last = stage == STAGES - 1
    lag = lag_of(stage)
    scale = 1.0 / (micro * tokens * width)

    def at_stage(pos):
        return {"stage": pos}

    def copy_w1():
        return pltpu.make_async_copy(w1_hbm.at[0], w1, wsem.at[0])

    def copy_w2():
        return pltpu.make_async_copy(w2_hbm.at[0], w2, wsem.at[1])

    def load_x(i):
        slot = lax.rem(i, RING)
        return pltpu.make_async_copy(x_hbm.at[i], xring.at[slot], xrecv.at[slot])

    def load_y(i):
        return pltpu.make_async_copy(y_hbm.at[i], ybuf.at[lax.rem(i, 2)], ysem.at[lax.rem(i, 2)])

    def send_x(i):
        return pltpu.make_async_remote_copy(
            src_ref=gring.at[G_RING + lax.rem(i, 2)], dst_ref=xring.at[lax.rem(i, RING)], send_sem=xsem.at[lax.rem(i, 2)],
            recv_sem=xrecv.at[lax.rem(i, RING)], device_id=at_stage(lax.rem(stage + 1, STAGES)), device_id_type=MESH)

    def send_g(i):
        return pltpu.make_async_remote_copy(
            src_ref=gsend.at[lax.rem(i, 2)], dst_ref=gring.at[lax.rem(i, G_RING)], send_sem=gsem.at[lax.rem(i, 2)],
            recv_sem=grecv.at[lax.rem(i, G_RING)], device_id=at_stage(lax.rem(stage + STAGES - 1, STAGES)),
            device_id_type=MESH)

    def save_nt(i):
        return pltpu.make_async_copy(ntbuf.at[lax.rem(i, 2)], nt_hbm.at[i], ntsem.at[lax.rem(i, 2)])

    def save_a(i):
        return pltpu.make_async_copy(abuf.at[lax.rem(i, 2)], a_hbm.at[i], asem.at[lax.rem(i, 2)])

    def save_d(i):
        return pltpu.make_async_copy(dbuf.at[lax.rem(i, 2)], d_hbm.at[i], dosem.at[lax.rem(i, 2)])

    def load_d(i):
        return pltpu.make_async_copy(d_hbm.at[i], dbuf.at[2 + lax.rem(i, 2)], disem.at[lax.rem(i, 2)])

    def save_du(i):
        return pltpu.make_async_copy(dubuf.at[lax.rem(i, 2)], du_hbm.at[i], dusem.at[lax.rem(i, 2)])

    def save_gt(i):
        return pltpu.make_async_copy(gtbuf.at[lax.rem(i, 2)], gt_hbm.at[i], gtsem.at[lax.rem(i, 2)])

    def load_wnt(i):
        return pltpu.make_async_copy(nt_hbm.at[i], wnt, wlsem.at[0])

    def load_wa(i):
        return pltpu.make_async_copy(a_hbm.at[i], wa, wlsem.at[1])

    def save_acc():
        return pltpu.make_async_copy(acc, acc_hbm, accsem)

    copy_w1().start()
    copy_w2().start()

    @pl.when(first)
    def _():
        load_x(0).start()

    load_y(0).start()
    barrier = pltpu.get_barrier_semaphore()
    for step in range(1, STAGES):
        pl.semaphore_signal(barrier, inc=1, device_id=at_stage(lax.rem(stage + step, STAGES)), device_id_type=MESH)
    gg_ref[...] = jnp.zeros_like(gg_ref)
    lbuf[...] = jnp.zeros_like(lbuf)

    def clear(row, carry):
        for part in range(2):
            acc[part, pl.ds(pl.multiple_of(row * 8, 8), 8), :] = jnp.zeros((8, hidden), F32)
        return carry

    lax.fori_loop(0, width // 8, clear, 0)
    pl.semaphore_wait(barrier, STAGES - 1)

    copy_w1().wait()
    copy_w2().wait()

    def normalize(i, slot, two):
        gain = gain_ref[...]
        for row in range(0, tokens, ROWS):
            x_f = xring[slot, row:row + ROWS, :].astype(F32)
            inv = lax.rsqrt(jnp.mean(x_f * x_f, axis=-1, keepdims=True) + NORM_EPS)
            nbuf[row:row + ROWS, :] = (x_f * inv * gain).astype(BF16)
        ntbuf[two] = nbuf[...].T

    def expand(two, col):
        u = jnp.dot(nbuf[...], w1[:, col:col + COLS], preferred_element_type=F32)
        u_sq = u * u
        th = jnp.tanh(u * (GELU_C + (GELU_C * GELU_A) * u_sq))
        h = 0.5 * th + 0.5
        abuf[two, :, col:col + COLS] = (u * h).astype(BF16)
        slope = u * (2.0 * GELU_C + (6.0 * GELU_C * GELU_A) * u_sq)
        dbuf[two, :, col:col + COLS] = h + (h - h * h) * slope

    def finish_forward(slot, two, ocol, update):
        out = (xring[slot, :, ocol].astype(F32) + update).astype(BF16)
        delta = out.astype(F32) - ybuf[two, :, ocol].astype(F32)
        gring[G_RING + two, :, ocol] = jnp.where(last, ((2.0 * scale) * delta).astype(BF16), out)
        lbuf[:, ocol] += jnp.sum((delta * delta).reshape(tokens // 8, 8, -1), axis=0)

    def grad_hidden(g_slot, d_slot, two, col):
        ga = lax.dot_general(gring[g_slot], w2[col:col + COLS, :], NT, preferred_element_type=F32)
        ga = ga.astype(BF16).astype(F32)
        dubuf[two, :, col:col + COLS] = (ga * dbuf[d_slot, :, col:col + COLS]).astype(BF16)

    def finish_backward(slot, g_slot, two, gn_all):
        gsend[two] = gn_all.astype(BF16)
        gain = gain_ref[...]
        for row in range(0, tokens, ROWS):
            x_f = xring[slot, row:row + ROWS, :].astype(F32)
            inv = lax.rsqrt(jnp.mean(x_f * x_f, axis=-1, keepdims=True) + NORM_EPS)
            x_hat = x_f * inv
            gn = gsend[two, row:row + ROWS, :].astype(F32)
            gg_ref[...] += jnp.sum((gn * x_hat).reshape(ROWS // 8, 8, width), axis=0)
            ghat = gn * gain
            gx = inv * (ghat - x_hat * jnp.mean(ghat * x_hat, axis=-1, keepdims=True))
            gsend[two, row:row + ROWS, :] = (gring[g_slot, row:row + ROWS, :].astype(F32) + gx).astype(BF16)

    def compute(do_f, do_b, i, j):
        f_slot, f_two = lax.rem(i, RING), lax.rem(i, 2)
        b_slot, b_two = lax.rem(j, RING), lax.rem(j, 2)
        d_slot = jnp.where(last, b_two, 2 + b_two)
        g_slot = jnp.where(last, G_RING + b_two, lax.rem(j, G_RING))
        blocks = range(hidden // COLS)
        if do_f:
            normalize(i, f_slot, f_two)
        gn_all = None
        update = None
        for kind, k in ORDER if do_b else FORWARD_ORDER:
            if kind == "A":
                part = jnp.dot(abuf[f_two, :, k * COLS:(k + 1) * COLS], w2[k * COLS:(k + 1) * COLS, :],
                               preferred_element_type=F32)
                update = part if update is None else update + part
            if kind == "Z":
                finish_forward(f_slot, f_two, slice(0, width), update)
            if kind == "E" and do_f:
                expand(f_two, k * COLS)
            if kind == "G" and do_b:
                grad_hidden(g_slot, d_slot, b_two, k * COLS)
            if kind == "N" and do_b:
                part = lax.dot_general(dubuf[b_two, :, k * COLS:(k + 1) * COLS], w1[:, k * COLS:(k + 1) * COLS], NT,
                                       preferred_element_type=F32)
                gn_all = part if gn_all is None else gn_all + part
            if kind == "B" and do_b:
                gtbuf[b_two] = gring[g_slot].T
                finish_backward(b_slot, g_slot, b_two, gn_all)
            if kind == "U" and do_f:
                ocol = slice(k * OUTC, (k + 1) * OUTC)
                update = jnp.dot(abuf[f_two], w2[:, ocol], preferred_element_type=F32)
                finish_forward(f_slot, f_two, ocol, update)

    def weight_grads(j):
        two = lax.rem(j, 2)
        load_wnt(j).wait()
        load_wa(j).wait()
        for col in range(0, hidden, WCOLS):
            block = slice(col, col + WCOLS)
            acc[0, :, block] += jnp.dot(wnt[...], dubuf[two, :, block], preferred_element_type=F32)
            acc[1, :, block] += jnp.dot(gtbuf[two], wa[:, block], preferred_element_type=F32)

    def before_forward(i):
        @pl.when(first)
        def _():
            load_x(i).wait()

            @pl.when(i + 1 < micro)
            def _():
                load_x(i + 1).start()

        @pl.when(jnp.logical_not(first))
        def _():
            send_x(i).wait_recv()

        load_y(i).wait()

        @pl.when(i + 1 < micro)
        def _():
            load_y(i + 1).start()

    def after_forward(i):
        save_nt(i).start()
        save_a(i).start()

        @pl.when(jnp.logical_not(last))
        def _():
            save_d(i).start()
            send_x(i).start()

    def before_backward(j):
        @pl.when(jnp.logical_not(last))
        def _():
            load_d(j).wait()
            send_g(j).wait_recv()

    def after_backward(j):
        save_du(j).start()
        save_gt(j).start()

        @pl.when(jnp.logical_not(last) & (j < micro - G_RING))
        def _():
            pl.semaphore_signal(gfree, inc=1, device_id=at_stage(lax.rem(stage + 1, STAGES)), device_id_type=MESH)

        @pl.when(jnp.logical_not(first) & (j >= G_RING))
        def _():
            pl.semaphore_wait(gfree, 1)

        @pl.when(jnp.logical_not(first))
        def _():
            send_g(j).start()

    def tick(t, carry):
        i = t
        j = t - lag
        f_on = i < micro
        b_on = (j >= 0) & (j < micro)

        @pl.when((i >= 2) & (i < micro + 2))
        def _():
            save_nt(i - 2).wait()
            save_a(i - 2).wait()

            @pl.when(jnp.logical_not(last))
            def _():
                save_d(i - 2).wait()
                send_x(i - 2).wait_send()

        @pl.when((j >= 2) & (j < micro + 2))
        def _():
            save_du(j - 2).wait()
            save_gt(j - 2).wait()

            @pl.when(jnp.logical_not(first))
            def _():
                send_g(j - 2).wait_send()

        @pl.when(f_on)
        def _():
            before_forward(i)

        @pl.when(b_on)
        def _():
            before_backward(j)

        @pl.when(jnp.logical_not(last) & (j + 1 >= 0) & (j + 1 < micro))
        def _():
            load_d(j + 1).start()

        w_on = jnp.logical_not(f_on) & (j < micro - SKIP)

        @pl.when(w_on)
        def _():
            load_wnt(j).start()
            load_wa(j).start()

        @pl.when(jnp.logical_not(last) & (j == micro - SKIP))
        def _():
            save_acc().start()

        @pl.when(f_on & b_on)
        def _():
            compute(True, True, i, j)

        @pl.when(f_on & jnp.logical_not(b_on))
        def _():
            compute(True, False, i, j)

        @pl.when(b_on & jnp.logical_not(f_on))
        def _():
            compute(False, True, i, j)

        @pl.when(b_on)
        def _():
            after_backward(j)

        @pl.when(f_on)
        def _():
            after_forward(i)

        @pl.when(w_on)
        def _():
            weight_grads(j)

        return carry

    lax.fori_loop(0, micro + LAGS[0] + 2, tick, 0)

    @pl.when(jnp.logical_not(last))
    def _():
        save_acc().wait()

    def send_loss(pos):
        return pltpu.make_async_remote_copy(
            src_ref=lbuf, dst_ref=lbuf, send_sem=lsend.at[pos], recv_sem=lrecv, device_id=at_stage(pos),
            device_id_type=MESH)

    @pl.when(last)
    def _():
        for pos in range(STAGES - 1):
            send_loss(pos).start()
        for pos in range(STAGES - 1):
            send_loss(pos).wait_send()

    @pl.when(jnp.logical_not(last))
    def _():
        send_loss(0).wait_recv()

    loss_ref[...] = lbuf[...]


def run_pipeline(x_in, y_target, w_up, w_down, gain):
    micro, tokens, width = x_in.shape
    hidden = w_up.shape[2]
    any_spec = pl.BlockSpec(memory_space=pl.ANY)
    vmem_spec = pl.BlockSpec(memory_space=pltpu.VMEM)
    dma = pltpu.SemaphoreType.DMA
    return pl.pallas_call(
        pipeline_kernel,
        out_shape=(
            jax.ShapeDtypeStruct((micro, width, tokens), BF16),
            jax.ShapeDtypeStruct((micro, tokens, hidden), BF16),
            jax.ShapeDtypeStruct((micro, tokens, hidden), BF16),
            jax.ShapeDtypeStruct((micro, width, tokens), BF16),
            jax.ShapeDtypeStruct((micro, tokens, hidden), F32),
            jax.ShapeDtypeStruct((2, width, hidden), F32),
            jax.ShapeDtypeStruct((8, width), F32),
            jax.ShapeDtypeStruct((8, width), F32),
        ),
        in_specs=[any_spec, any_spec, any_spec, any_spec, vmem_spec],
        out_specs=(any_spec, any_spec, any_spec, any_spec, any_spec, any_spec, vmem_spec, vmem_spec),
        scratch_shapes=[
            pltpu.VMEM((width, hidden), BF16),
            pltpu.VMEM((hidden, width), BF16),
            pltpu.VMEM((RING, tokens, width), BF16),
            pltpu.VMEM((G_RING + 2, tokens, width), BF16),
            pltpu.VMEM((2, tokens, width), BF16),
            pltpu.VMEM((tokens, width), BF16),
            pltpu.VMEM((2, width, tokens), BF16),
            pltpu.VMEM((2, width, tokens), BF16),
            pltpu.VMEM((2, tokens, hidden), BF16),
            pltpu.VMEM((4, tokens, hidden), F32),
            pltpu.VMEM((2, tokens, hidden), BF16),
            pltpu.VMEM((2, tokens, width), BF16),
            pltpu.VMEM((2, width, hidden), F32),
            pltpu.VMEM((width, tokens), BF16),
            pltpu.VMEM((tokens, hidden), BF16),
            pltpu.VMEM((8, width), F32),
            dma((2,)), dma((RING,)), dma((G_RING,)), dma((2,)), dma((2,)), dma((2,)), dma((2,)), dma((2,)), dma((2,)),
            dma((2,)), dma((2,)), dma((2,)), dma((2,)), dma, dma((STAGES - 1,)), dma, pltpu.SemaphoreType.REGULAR,
        ],
        compiler_params=pltpu.CompilerParams(
            collective_id=0, has_side_effects=True,
            vmem_limit_bytes=67043328),
        cost_estimate=pl.CostEstimate(
            flops=8 * micro * tokens * width * hidden, transcendentals=micro * tokens * hidden,
            bytes_accessed=16 * micro * tokens * hidden),
        name="pipeline",
    )(x_in, y_target, w_up, w_down, gain)


def weight_kernel(scale, nt_hbm, gt_hbm, du_hbm, a_hbm, acc_hbm, gg_ref, loss_rows,
                  up_hbm, down_hbm, gain_out, loss_out, lhs, rhs, prev, up_out, down_out, lsem, rsem, psem, osem):
    micro, width, tokens = nt_hbm.shape
    hidden = du_hbm.shape[2]
    rounds = hidden // WIDE
    half = WIDE // 2
    rows = width // 2
    lag = lag_of(lax.axis_index("stage"))
    has_prev = lag > 1
    cut = micro - jnp.where(has_prev, lag, SKIP)
    count = cut + SKIP

    def source(k):
        return jnp.where(k < cut, k, micro - SKIP + k - cut)

    def load_lhs(part, k):
        return pltpu.make_async_copy((nt_hbm, gt_hbm)[part].at[source(k)], lhs.at[part, k], lsem.at[part, k])

    def load_rhs(part, pair, k):
        cols = pl.ds(pl.multiple_of(pair * WIDE, WIDE), WIDE)
        buf = lax.rem(pair, 2)
        return pltpu.make_async_copy((du_hbm, a_hbm)[part].at[source(k), :, cols], rhs.at[buf, k], rsem.at[buf, k])

    def load_prev(part, pair):
        cols = pl.ds(pl.multiple_of(pair * WIDE, WIDE), WIDE)
        buf = lax.rem(pair, 2)
        return pltpu.make_async_copy(acc_hbm.at[part, :, cols], prev.at[buf], psem.at[buf])

    def save(part, pair):
        start = pl.multiple_of(pair * WIDE, WIDE)
        buf = lax.rem(pair, 2)
        if part == 0:
            return pltpu.make_async_copy(up_out.at[buf], up_hbm.at[:, pl.ds(start, WIDE)], osem.at[0, buf])
        return pltpu.make_async_copy(down_out.at[buf], down_hbm.at[pl.ds(start, WIDE), :], osem.at[1, buf])

    def fetch(part, pair):
        load_prev(part, pair).start()

        def one(k, carry):
            load_rhs(part, pair, k).start()
            return carry

        lax.fori_loop(0, count, one, 0)

    def body(top_a, top_b, low_a, low_b):
        tops, lows = (top_a, top_b), (low_a, low_b)

        def first_loads(k, carry):
            load_lhs(0, k).start()
            load_rhs(0, 0, k).start()
            return carry

        lax.fori_loop(0, count, first_loads, 0)
        load_prev(0, 0).start()
        gain_out[...] = jnp.sum(gg_ref[...], axis=0, keepdims=True)
        loss_out[0] = jnp.sum(loss_rows[...]) * scale
        for accs, first_row in ((tops, 0), (lows, rows)):
            for side, acc in enumerate(accs):
                up_out[1, first_row:first_row + rows, side * half:(side + 1) * half] = pltpu.matmul_pop(acc)

        def drain(part, buf, low):
            first_row = rows if low else 0
            for side, acc in enumerate(lows if low else tops):
                cols = slice(side * half, (side + 1) * half)
                before = jnp.where(has_prev, prev[buf, first_row:first_row + rows, cols], 0.0)
                total = pltpu.matmul_pop(acc) + before
                if part == 0:
                    up_out[buf, first_row:first_row + rows, cols] = total
                else:
                    down_out[buf, cols, first_row:first_row + rows] = total.T

        def push(buf, k):
            pltpu.matmul_push_rhs(rhs[buf, k, :, 0:half], staging_register=0, mxu_index=0)
            pltpu.matmul_push_rhs(rhs[buf, k, :, half:WIDE], staging_register=0, mxu_index=1)

        def multiply_top(part, k):
            left = lhs[part, k, 0:rows, :]
            for acc in tops:
                pltpu.matmul_acc_lhs(acc, left, load_staged_rhs=0)

        def multiply_low(part, k):
            left = lhs[part, k, rows:width, :]
            for acc in lows:
                pltpu.matmul_acc_lhs(acc, left)

        for part in range(2):
            def one_round(pair, carry, part=part):
                buf = lax.rem(pair, 2)

                def arrive(k):
                    load_rhs(part, pair, k).wait()

                    @pl.when(pair == 0)
                    def _():
                        load_lhs(part, k).wait()

                def start_round(drain_part, drain_buf):
                    multiply_top(part, 0)
                    if drain_part is not None:
                        drain(drain_part, drain_buf, True)
                    push(buf, 1)
                    multiply_low(part, 0)

                def step(k):
                    multiply_top(part, k)
                    push(buf, k + 1)
                    multiply_low(part, k)

                def two_steps(i, carry):
                    k = 1 + 2 * i
                    arrive(k + 1)
                    arrive(k + 2)
                    step(k)
                    step(k + 1)
                    return carry

                arrive(0)
                arrive(1)

                push(buf, 0)

                @pl.when(pair == 0)
                def _():
                    if part == 0:
                        start_round(None, None)
                    else:
                        start_round(0, (rounds - 1) % 2)
                        save(0, rounds - 1).start()

                @pl.when(pair > 0)
                def _():
                    start_round(part, 1 - buf)
                    save(part, pair - 1).start()

                @pl.when(pair + 1 < rounds)
                def _():
                    fetch(part, pair + 1)

                if part == 0:
                    @pl.when(pair == rounds - 1)
                    def _():
                        fetch(1, 0)

                    @pl.when(pair == 2)
                    def _():
                        def more(k, carry):
                            load_lhs(1, k).start()
                            return carry

                        lax.fori_loop(0, count, more, 0)

                lax.fori_loop(0, (count - 2) // 2, two_steps, 0)

                @pl.when(lax.rem(count, 2) == 1)
                def _():
                    arrive(count - 1)
                    step(count - 2)

                load_prev(part, pair).wait()

                @pl.when(pair >= 2)
                def _():
                    save(part, pair - 2).wait()

                multiply_top(part, count - 1)
                multiply_low(part, count - 1)
                drain(part, buf, False)
                return carry

            lax.fori_loop(0, rounds, one_round, 0)
        drain(1, (rounds - 1) % 2, True)
        save(1, rounds - 1).start()
        for part in range(2):
            for pair in range(rounds - 2, rounds):
                save(part, pair).wait()

    shape = (rows, half)
    pl.run_scoped(
        body, pltpu.ACC(0)(shape, F32), pltpu.ACC(1)(shape, F32), pltpu.ACC(0)(shape, F32), pltpu.ACC(1)(shape, F32))


def run_weights(nt_all, gt_all, du_all, a_all, acc, gain_rows, loss_rows):
    micro, width, tokens = nt_all.shape
    hidden = du_all.shape[2]
    any_spec = pl.BlockSpec(memory_space=pl.ANY)
    vmem_spec = pl.BlockSpec(memory_space=pltpu.VMEM)
    dma = pltpu.SemaphoreType.DMA
    return pl.pallas_call(
        functools.partial(weight_kernel, 1.0 / (micro * tokens * width)),
        out_shape=(
            jax.ShapeDtypeStruct((width, hidden), F32),
            jax.ShapeDtypeStruct((hidden, width), F32),
            jax.ShapeDtypeStruct((1, width), F32),
            jax.ShapeDtypeStruct((1,), F32),
        ),
        in_specs=[any_spec] * 5 + [vmem_spec] * 2,
        out_specs=(any_spec, any_spec, vmem_spec, pl.BlockSpec(memory_space=pltpu.SMEM)),
        scratch_shapes=[
            pltpu.VMEM((2, micro, width, tokens), BF16),
            pltpu.VMEM((2, micro, tokens, WIDE), BF16),
            pltpu.VMEM((2, width, WIDE), F32),
            pltpu.VMEM((2, width, WIDE), F32),
            pltpu.VMEM((2, WIDE, width), F32),
            dma((2, micro)), dma((2, micro)), dma((2,)), dma((2, 2)),
        ],
        compiler_params=pltpu.CompilerParams(vmem_limit_bytes=67043328),
        cost_estimate=pl.CostEstimate(
            flops=4 * micro * tokens * width * hidden, transcendentals=0, bytes_accessed=4 * micro * tokens * hidden),
        name="weights",
    )(nt_all, gt_all, du_all, a_all, acc, gain_rows, loss_rows)


def solution(mesh):
    def device_step(x_in, y_target, w_up, w_down, gain):
        nt_all, a_all, du_all, gt_all, _, acc, gain_rows, loss_rows = run_pipeline(x_in, y_target, w_up, w_down, gain)
        grad_up, grad_down, grad_gain, loss = run_weights(nt_all, gt_all, du_all, a_all, acc, gain_rows, loss_rows)
        return loss, grad_up[None], grad_down[None], grad_gain

    weight_spec = P("stage", None, None)
    grad_spec = P(("data", "stage"), None, None)
    return jax.shard_map(
        device_step, mesh=mesh,
        in_specs=(P("data", None, None), P("data", None, None), weight_spec, weight_spec, P("stage", None)),
        out_specs=(P("data"), grad_spec, grad_spec, P(("data", "stage"), None)), check_vma=False)
```
